256 devices in a mesh: groups: 2 (over z), ep: 16 (over x, core), tp: 8 (over y).
Axes of the slice: x: 8, y: 8, z: 2, core: 2. Of those that a mesh axis runs over, the one named last changes fastest.
The devices are a block of a 8x8x16 slice.
Arguments:
- tokens: bfloat16 [1024, 7168], P(('groups', 'ep')), parts along dimension 0, may hold values from -6 to 6
- w_gate: bfloat16 [16, 7168, 2048], P('ep', None, 'tp'), may hold values from -0.0625 to 0.0625
- w_up: bfloat16 [16, 7168, 2048], P('ep', None, 'tp'), may hold values from -0.0625 to 0.0625
- w_down: bfloat16 [16, 2048, 7168], P('ep', 'tp'), may hold values from -0.1875 to 0.1875
- router_logits: float32 [1024, 8], P(('groups', 'ep')), parts along dimension 0, may hold values from -6 to 6
- expert_ids: int32 [1024, 8], P(('groups', 'ep')), parts along dimension 0, may hold values from 0 to 15, all different within a row; in each aligned block of 32 rows (0 to 31, 32 to 63, ...) at most 24 rows name the same one
- draft_lengths: int32 [128], P(('groups', 'ep')), parts along dimension 0, may hold values from 7 to 8
- accept_mask: int32 [128, 8], P(('groups', 'ep')), parts along dimension 0, may hold values 0 or 1
Outputs:
- mixed: bfloat16 [1024, 7168], P(('groups', 'ep'), 'tp'), parts along dimension 0
- accepted: int32 [2], P('groups'), parts along dimension 0
The draws below stay inside these ranges and needn't reach their ends.
There are 2 independent parts, one for each index of `groups`. The reference program is written for one: setup_inputs(seed, part) draws one part's arguments, and reference() takes and returns one part's arrays. A program takes and returns all parts, laid end to end along the dimension named above; an argument that names none is the same for every part. Nothing has to cross between parts.
Inputs may be any that keep to these rules, and one draw needn't show every extreme that they name: `expert_ids`: each row names 8 different experts. Among the rows of one ep index (aligned blocks of 32 rows) no expert is named by more than 24 rows, and in every draw some expert is named by exactly 24 rows of some block.
All inputs are finite; a program needn't handle non-finite values. No bound on the sum of `accept_mask` on one device may be relied on, other than what follows from the above.
Results may differ from the reference program's by a relative error of at most 0.017.
Values may be sent and summed in bfloat16 or wider, within the bound.
A program may use at most 128 MiB of HBM per device.

```python
import math
import jax
import jax.numpy as jnp
import numpy as np
from jax import lax

D = 7168
FF = 2048
TOP = 8
DRAFT = 8
EXPERTS = 16
TOK_DEV = 32
REQUESTS = 64
TOKENS = 512
CAP = 24
N_EP = 16
N_TP = 8


def set_ends(result, own_key, smallest, high):
    shape = result.shape
    spot = [jax.random.randint(jax.random.fold_in(own_key, axis), (), 0, shape[axis]) for axis in range(len(shape))]
    result = result.at[tuple(spot)].set(smallest)
    longest = shape.index(max(shape))
    spot[longest] = (spot[longest] + 1) % shape[longest]
    return result.at[tuple(spot)].set(high)


def raised(entries, rng, source, target, blocks, factor):
    owner, partner = [(jnp.arange(entries.shape[position]) // (entries.shape[position] // blocks)).reshape([-1 if axis == position else 1 for axis in range(entries.ndim)]) for position in (source, target)]
    chosen = jax.random.permutation(rng, blocks)[partner]
    strong = (owner == chosen) | (owner == (partner + blocks // 2) % blocks)
    return jnp.where(strong, factor * entries, entries)


def block_levels(own_key, extent, shards, low, high):
    gain, own = 1.0, jax.random.fold_in(own_key, 6)
    for axis_at, blocks in shards:
        draws = jnp.exp(jax.random.uniform(jax.random.fold_in(own, axis_at), (blocks,), jnp.float32, low / len(shards), high / len(shards)))
        gain = gain * jnp.repeat(draws, extent[axis_at] // blocks).reshape([-1 if axis == axis_at else 1 for axis in range(len(extent))])
    return gain


def shared_out(own_key, own, number, rows, count, top, reach, lean):
    order = jax.random.permutation(own_key, count)
    heavy_load, common = shares(count, rows * top, reach, lean, True), shares(count, rows * top, reach, lean, False)
    places = jnp.arange(count)

    def named(tallies, rotation):
        used = int((tallies > 0).sum())
        fixed = max(1, used // 4)
        shifted = fixed + (places - fixed + rotation * (used - fixed)) % max(1, count - fixed)
        return jnp.zeros((count,), jnp.int32).at[order[jnp.where(places < fixed, places, shifted)]].set(jnp.asarray(tallies, jnp.int32))

    tallies = jnp.where(number % 4 == 0, named(heavy_load, number // 4), named(common, number - number // 4 - 1))
    mixed = jax.random.permutation(jax.random.fold_in(own, 3), count)
    giver, taker = mixed[0:count // 2 * 2:2], mixed[1:count // 2 * 2:2]
    slack = jnp.minimum(tallies[giver] - 1, reach - tallies[taker]) // 2
    slack = jnp.where((giver == order[0]) | (taker == order[0]) | (tallies[taker] == 0), 0, jnp.maximum(slack, 0))
    shifted = jax.random.randint(jax.random.fold_in(own, 4), (count // 2,), 0, 1 << 20) % (slack + 1)
    tallies = tallies.at[giver].add(-shifted).at[taker].add(shifted)
    labels = jnp.searchsorted(jnp.cumsum(tallies), jnp.arange(rows * top), side="right").astype(jnp.int32)
    listing = labels.reshape(top, rows).T
    listing = listing[jax.random.permutation(jax.random.fold_in(own, 1), rows)]
    rotation = jax.random.randint(jax.random.fold_in(own, 2), (rows, 1), 0, top)
    return jnp.take_along_axis(listing, (jnp.arange(top)[None, :] + rotation) % top, axis=1)


def shares(amount, total, limit, skew, full):
    loads = [(1 << 20) // math.isqrt(rank ** skew) + 1 for rank in range(1, amount + 1)]
    largest = limit if full else min(limit, max(-(-total // amount), total * loads[0] // sum(loads)))
    least = 1 if total - largest >= amount - 1 else 0
    given, surplus = [largest] + [least] * (amount - 1), total - largest - least * (amount - 1)
    while surplus > 0:
        movable = [i for i in range(1, amount) if given[i] < largest] or [i for i in range(1, amount) if given[i] < limit]
        whole, remaining = sum([loads[i] for i in movable]), surplus
        for i in movable:
            extra = min(limit - given[i], max(1, remaining * loads[i] // whole), surplus)
            given[i] = given[i] + extra
            surplus = surplus - extra
    return np.array(given)


def bell_draw(stream_key, shape, scale, bound, shards=(), held_as=jnp.bfloat16):
    values = jax.random.normal(stream_key, shape, jnp.float32) * scale
    if len(shards) > 0:
        values = block_levels(stream_key, shape, shards, -0.22, 0.18) * values
    return jnp.clip(values, min=-bound, max=bound).astype(held_as)


def gaussian_with(rng, shape, deviation, bound, shards, heavy, kind=jnp.bfloat16):
    drawn = deviation * jax.random.normal(rng, shape, jnp.float32)
    if shards:
        drawn = drawn * block_levels(rng, shape, shards, -0.22, 0.18)
    return jnp.clip(raised(drawn, jax.random.fold_in(rng, 3), *heavy), -bound, bound).astype(kind)


def setup_inputs(seed: int = 0, part: int = 0) -> dict:
    arg_keys = jax.random.split(jax.random.key(seed), 9)
    own_keys = jax.random.split(jax.random.fold_in(arg_keys[8], part), 9)
    tokens = bell_draw(own_keys[0], (TOKENS, D), 1.0, 6.0, ((0, 16),))
    w_gate = bell_draw(arg_keys[1], (EXPERTS, D, FF), D ** -0.5, 0.0625, ((0, 16), (2, 8)))
    w_up = bell_draw(arg_keys[2], (EXPERTS, D, FF), D ** -0.5, 0.0625, ((0, 16), (2, 8)))
    w_down = gaussian_with(arg_keys[3], (EXPERTS, FF, D), FF ** -0.5, 0.1875, ((0, 16), (1, 8)), (1, 2, 8, 2.0))
    router_logits = bell_draw(own_keys[4], (TOKENS, TOP), 1.5, 6.0, ((0, 16),), jnp.float32)
    expert_ids_keys = jax.random.split(jax.random.fold_in(own_keys[5], 1), TOKENS // TOK_DEV)
    expert_ids_turns = jax.random.permutation(jax.random.fold_in(own_keys[5], 3), TOKENS // TOK_DEV)
    expert_ids = jax.vmap(lambda own, number: shared_out(jax.random.fold_in(own_keys[5], 2), own, number, TOK_DEV, EXPERTS, TOP, CAP, 2))(expert_ids_keys, expert_ids_turns).reshape((TOKENS, TOP))
    draft_lengths = set_ends(jax.random.randint(own_keys[6], (REQUESTS,), DRAFT - 1, DRAFT + 1), jax.random.fold_in(own_keys[6], 1), DRAFT - 1, DRAFT).astype(jnp.int32)
    accept_mask = set_ends((jax.random.randint(own_keys[7], (REQUESTS, DRAFT), 0, 4) < 3).astype(jnp.int32), jax.random.fold_in(own_keys[7], 1), 0, 1)
    return dict(tokens=tokens, w_gate=w_gate, w_up=w_up, w_down=w_down, router_logits=router_logits, expert_ids=expert_ids, draft_lengths=draft_lengths, accept_mask=accept_mask)


def reference(tokens, w_gate, w_up, w_down, router_logits, expert_ids, draft_lengths, accept_mask):
    live = jnp.arange(DRAFT, dtype=jnp.int32)[None, :] < draft_lengths[:, None]
    live_rows = live.reshape(TOKENS)
    live_tokens = jnp.where(live_rows[:, None], tokens, jnp.zeros((), tokens.dtype))
    sig = jax.nn.sigmoid(router_logits.astype(jnp.float32))
    gates = 2.827 * sig / jnp.sum(sig, axis=1, keepdims=True)
    load = N_EP * CAP
    flat_ids = expert_ids.reshape(-1).astype(jnp.int32)
    onehot = (flat_ids[:, None] == jnp.arange(EXPERTS, dtype=jnp.int32)[None, :]).astype(jnp.int32)
    rank = jnp.cumsum(onehot, axis=0) - 1
    slot = jnp.sum(rank * onehot, axis=1).astype(jnp.int32)
    source = (jnp.arange(TOKENS * TOP, dtype=jnp.int32) // TOP).astype(jnp.int32)
    table = jnp.zeros((EXPERTS, load), jnp.int32).at[flat_ids, slot].set(source)
    filled = jnp.zeros((EXPERTS, load), jnp.int32).at[flat_ids, slot].set(1)

    def one_expert(items):
        weight_g, weight_u, weight_d, rows_of, used = items
        rows = jnp.where(used[:, None] > 0, live_tokens[rows_of], jnp.zeros((), tokens.dtype))
        gate = jnp.dot(rows, weight_g, preferred_element_type=jnp.float32)
        up = jnp.dot(rows, weight_u, preferred_element_type=jnp.float32)
        hidden = (jax.nn.silu(gate) * up).astype(jnp.bfloat16)
        blocks = hidden.reshape(load, N_TP, FF // N_TP).astype(jnp.float32)
        down = weight_d.reshape(N_TP, FF // N_TP, D).astype(jnp.float32)
        parts = jnp.einsum('mtf,tfd->tmd', blocks, down)
        summed = jnp.sum(parts.astype(jnp.bfloat16).astype(jnp.float32), axis=0)
        return summed.astype(jnp.bfloat16)

    outs = lax.map(one_expert, (w_gate, w_up, w_down, table, filled))
    picked = outs[flat_ids, slot].reshape(TOKENS, TOP, D).astype(jnp.float32)
    mixed = jnp.sum(gates[:, :, None] * picked, axis=1).astype(jnp.bfloat16)
    passed = accept_mask.astype(jnp.int32) * live.astype(jnp.int32)
    prefix = jnp.cumprod(passed, axis=1)
    accepted = jnp.sum(prefix).astype(jnp.int32).reshape(1)
    return mixed, accepted
```

```python
import functools

import jax
import jax.numpy as jnp
from jax import lax
from jax.experimental import pallas as pl
from jax.experimental.pallas import tpu as pltpu
from jax.sharding import PartitionSpec as P

MESH = pl.DeviceIdType.MESH
DRAFT = 8
SCALE = 2.827
BF16, F32 = jnp.bfloat16, jnp.float32


def signed_order(n):
    half = n // 2
    order = [half]
    for d in range(half - 1, 0, -1):
        order += [d, -d]
    return order + [0]


def kernel(cfg, tok_ref, wg_ref, wu_ref, wd_ref, logit_ref, ids_ref, len_ref, mask_ref, out_ref, count_ref,
           X, G, WG, WU, WD, ACC, P1, P2, RB1, RB2, F1, F2, C,
           tok_sem, wl_sem, wr_send, wr_recv, ag_send, ag_recv, h1_send, h1_recv, h2_send, h2_recv,
           f1_send, f1_recv, f2_send, f2_recv, c_send, c_recv, d_sem, dr_send, dr_recv):
    NX, NY, NC = cfg["nx"], cfg["ny"], cfg["chunks"]
    HX, HY = NX // 2, NY // 2
    rows = cfg["rows"]
    half = rows // 2
    kc = cfg["kc"]
    ncol = cfg["ncol"]
    hid = cfg["hid"]
    nexp = cfg["nexp"]
    n_ep = 2 * NX
    ep = lax.axis_index("ep")
    tp = lax.axis_index("tp")
    core = lax.rem(ep, 2)
    partner = {"ep": ep + 1 - 2 * core}

    def xdev(d):
        return {"ep": lax.rem(ep + (2 * d) % n_ep, n_ep)}

    def ydev(d):
        return {"tp": lax.rem(tp + d % NY, NY)}

    kk = signed_order(NY)

    pending = []

    def remote(src, dst, send, recv, dev):
        c = pltpu.make_async_remote_copy(src_ref=src, dst_ref=dst, send_sem=send, recv_sem=recv,
                                         device_id=dev, device_id_type=MESH)
        c.start()
        pending.append(c)
        return c

    tok = []
    for q in range(NC):
        c = pltpu.make_async_copy(tok_ref.at[:, pl.ds(q * kc, kc)], X.at[q, 0], tok_sem.at[q])
        c.start()
        tok.append(c)
    wl = []
    for q in range(NC):
        r = pl.ds(q * kc, kc)
        for i, (src, dst) in enumerate(((wg_ref, WG), (wu_ref, WU))):
            c = pltpu.make_async_copy(src.at[0, r], dst.at[0, r], wl_sem.at[q, i])
            c.start()
            wl.append(c)
    dl = []
    dcols = []
    for p in range(NY):
        col = pl.ds(pl.multiple_of(lax.rem(tp + kk[p] % NY, NY) * ncol, 128), ncol)
        dcols.append(col)
        c = pltpu.make_async_copy(wd_ref.at[0, :, col], WD.at[p, pl.ds(0, hid)], d_sem.at[p])
        c.start()
        dl.append(c)

    barrier = pltpu.get_barrier_semaphore()
    peers = [partner] + [xdev(d) for d in range(1, NX)] + [ydev(d) for d in range(1, NY)]
    for dev in peers:
        pl.semaphore_signal(barrier, inc=1, device_id=dev, device_id_type=MESH)

    logits = logit_ref[...]
    sig = 1.0 / (1.0 + jnp.exp(-logits))
    gates = SCALE * sig / jnp.sum(sig, axis=0, keepdims=True)
    lane = lax.broadcasted_iota(jnp.int32, (1, rows), 1)
    length = jnp.zeros((1, rows), jnp.int32)
    for r in range(rows // DRAFT):
        length = jnp.where(lane // DRAFT == r, len_ref[r], length)
    gates = jnp.where(lane % DRAFT < length, gates, 0.0)
    mrow = lax.broadcasted_iota(jnp.int32, mask_ref.shape, 0)
    mcol = lax.broadcasted_iota(jnp.int32, mask_ref.shape, 1)
    mlen = jnp.zeros(mask_ref.shape, jnp.int32)
    for r in range(rows // DRAFT):
        mlen = jnp.where(mrow == r, len_ref[r], mlen)
    passed = jnp.where(mcol < mlen, mask_ref[...], 0).astype(F32)
    run = passed[:, 0:1]
    local_count = run
    for j in range(1, DRAFT):
        run = run * passed[:, j:j + 1]
        local_count = local_count + run
    local_count = jnp.sum(local_count, axis=0, keepdims=True)
    feat = lax.broadcasted_iota(jnp.int32, (128, rows), 0)
    dense = jnp.zeros((128, rows), F32)
    ids = ids_ref[...]
    for k in range(ids.shape[0]):
        e = ids[k:k + 1, :]
        dense = dense + jnp.where((feat == e) | (feat == e + nexp), gates[k:k + 1, :], 0.0)
    high = dense.astype(BF16)
    packed = jnp.where(feat < nexp, high.astype(F32), dense - high.astype(F32))
    packed = packed + jnp.where(feat == 2 * nexp, local_count, 0.0)
    eye = (lax.broadcasted_iota(jnp.int32, (rows, rows), 0) == lax.broadcasted_iota(jnp.int32, (rows, rows), 1))
    turned = lax.dot_general(eye.astype(F32).astype(BF16), packed.astype(BF16), (((1,), (1,)), ((), ())),
                             preferred_element_type=F32)
    G[0] = turned.astype(BF16)

    pl.semaphore_wait(barrier, len(peers))

    wr = []
    for q in range(NC):
        r = pl.ds(q * kc, kc)
        for i, (src, dst) in enumerate(((wg_ref, WG), (wu_ref, WU))):
            wr.append(remote(src.at[0, r], dst.at[1, r], wr_send.at[q, i], wr_recv.at[q, i], partner))
    dr = []
    for p in range(NY):
        dr.append(remote(wd_ref.at[0, :, dcols[p]], WD.at[p, pl.ds(hid, hid)], dr_send.at[p], dr_recv.at[p], partner))

    ag = {}
    lo, hi = pl.ds(0, half), pl.ds(half, half)

    def view(q, slot, part):
        ref = G.at[slot] if q == NC else X.at[q, slot]
        return ref if part is None else ref.at[part]

    def ag_send_step(q, s):
        if s == 0:
            if q < NC:
                tok[q].wait()
        else:
            ag[q, s - 1, 0].wait_recv()
        ag[q, s, 0] = remote(view(q, s, lo if s == HX - 1 else None), view(q, s + 1, lo if s == HX - 1 else None),
                             ag_send.at[q, s, 0], ag_recv.at[q, s, 0], xdev(1))
        if s > 0:
            ag[q, s - 1, 1].wait_recv()
        a, b = (NX - s) % NX, NX - s - 1
        ag[q, s, 1] = remote(view(q, a, hi if s == HX - 1 else None), view(q, b, hi if s == HX - 1 else None),
                             ag_send.at[q, s, 1], ag_recv.at[q, s, 1], xdev(-1))

    def ag_finish(q):
        ag[q, HX - 1, 0].wait_recv()
        ag[q, HX - 1, 1].wait_recv()

    def gate_up(q):
        r = pl.ds(q * kc, kc)
        x = X[q].reshape(NX * rows, kc)
        for i, w in enumerate((WG, WU)):
            for e in range(2):
                (wl if e == 0 else wr)[2 * q + i].wait() if e == 0 else wr[2 * q + i].wait_recv()
                y = jnp.dot(x, w[e, r, :], preferred_element_type=F32)
                if q == 0:
                    ACC[i, e] = y
                else:
                    ACC[i, e] = ACC[i, e] + y

    first = NC // 2
    groups = [list(range(first)), list(range(first, NC)) + [NC]]
    for s in range(HX):
        for q in groups[0]:
            ag_send_step(q, s)
    for s in range(HX):
        for n, q in enumerate(groups[1]):
            ag_send_step(q, s)
        if s < len(groups[0]):
            ag_finish(groups[0][s])
            gate_up(groups[0][s])
    for q in groups[0][HX:]:
        ag_finish(q)
        gate_up(q)
    for q in groups[1]:
        ag_finish(q)
        if q < NC:
            gate_up(q)

    g_all = G[...].reshape(NX * rows, 128).astype(F32)
    glane = lax.broadcasted_iota(jnp.int32, (NX * rows, 128), 1)
    grow = lax.broadcasted_iota(jnp.int32, (NX * rows, 128), 0)
    tally = jnp.where((glane == 2 * nexp) & (grow % rows == 0), g_all, 0.0)
    C[0] = jnp.zeros((8, 128), F32) + jnp.sum(tally)
    c_copy = remote(C.at[0], C.at[1], c_send, c_recv, partner)
    hs = []
    for e in range(2):
        expert = ep if e == 0 else partner["ep"]
        gate = jnp.sum(jnp.where((glane == expert) | (glane == expert + nexp), g_all, 0.0), axis=1, keepdims=True)
        g, u = ACC[0, e], ACC[1, e]
        hs.append((gate * (g / (1.0 + jnp.exp(-g)) * u)).astype(BF16))
    h = jnp.concatenate(hs, axis=1)

    def down(p):
        dl[p].wait()
        dr[p].wait_recv()
        y = jnp.dot(h, WD[p], preferred_element_type=F32).astype(BF16).reshape(NX, rows, ncol)
        P1[p] = y[:, :half]
        P2[p] = y[:, half:]

    pos = {k: p for p, k in enumerate(kk)}
    NQ = NY // 2
    NJ = NX // 2
    h1, h2 = {}, {}

    def add(dst, src):
        dst[...] = (dst[...].astype(F32) + src[...].astype(F32)).astype(BF16)

    def h1_step(q, s):
        for d in range(2):
            slot = (HX + s) % NX if d == 0 else HX - s
            if s == 0:
                p, n = 2 * q + d, 1
            else:
                p, n = 2 * q, 2
                h1[q, s - 1, d].wait_recv()
                pa, na = (2 * q + d, 1) if s == 1 else (p, n)
                add(P1.at[pl.ds(pa, na), slot], RB1.at[d, s - 1, pl.ds(pa, na)])
            h1[q, s, d] = remote(P1.at[pl.ds(p, n), slot], RB1.at[d, s, pl.ds(p, n)],
                                 h1_send.at[q, s, d], h1_recv.at[q, s, d], xdev(1 if d == 0 else -1))

    def h2_step(j, s):
        for d in range(2):
            p = pos[HY - s] if (d == 0 or s == 0) else pos[s - HY]
            mine = (j < NJ // 2) == (d == 0)
            rng = pl.ds(2 * j, 2)
            if s == 0 and not mine:
                continue
            if s > 0 and (s > 1 or mine):
                h2[j, s - 1, d].wait_recv()
                add(P2.at[p, rng], RB2.at[d, s - 1, rng])
            h2[j, s, d] = remote(P2.at[p, rng], RB2.at[d, s, rng],
                                 h2_send.at[j, s, d], h2_recv.at[j, s, d], ydev(1 if d == 0 else -1))

    down(0)
    for j in range(NJ):
        h2_step(j, 0)
    down(1)
    h1_step(0, 0)
    for q in range(1, NQ):
        down(2 * q)
        down(2 * q + 1)
        h1_step(q, 0)
        if q == 1:
            for j in range(NJ):
                h2_step(j, 1)
    for s in range(1, HX):
        for i in range(max(NQ, NJ)):
            if i < NQ:
                h1_step(i, s)
            if i < NJ and s + 1 < HY:
                h2_step(i, s + 1)

    f1, f2 = [], []
    last = NY - 1

    def h1_final(q):
        h1[q, HX - 1, 0].wait_recv()
        h1[q, HX - 1, 1].wait_recv()
        r = pl.ds(2 * q, 2)
        P1[r, 0] = (P1[r, 0].astype(F32) + RB1[0, HX - 1, r].astype(F32) + RB1[1, HX - 1, r].astype(F32)).astype(BF16)
        for p in (2 * q, 2 * q + 1):
            if kk[p] != 0:
                f1.append(remote(P1.at[p, 0], F1.at[p], f1_send.at[p], f1_recv.at[p], ydev(kk[p])))

    def h2_final(j):
        h2[j, HY - 1, 0].wait_recv()
        h2[j, HY - 1, 1].wait_recv()
        r = pl.ds(2 * j, 2)
        P2[last, r] = (P2[last, r].astype(F32) + RB2[0, HY - 1, r].astype(F32) + RB2[1, HY - 1, r].astype(F32)).astype(BF16)
        for slot in (2 * j, 2 * j + 1):
            if slot != 0:
                f2.append(remote(P2.at[last, slot], F2.at[slot], f2_send.at[slot], f2_recv.at[slot], xdev(-slot)))

    for i in range(max(NQ, NJ)):
        if i < NJ:
            h2_final(i)
        if i < NQ:
            h1_final(i)

    for c in f1 + f2:
        c.wait_recv()
    a = P1[last, 0].astype(F32)
    for p in range(NY):
        if kk[p] != 0:
            a = a + F1[p].astype(F32)
    out_ref[pl.ds(0, half), :] = a.astype(BF16)
    b = P2[last, 0].astype(F32)
    for slot in range(1, NX):
        b = b + F2[slot].astype(F32)
    out_ref[pl.ds(half, half), :] = b.astype(BF16)
    c_copy.wait_recv()
    first_only = ((lax.broadcasted_iota(jnp.int32, (8, 128), 0) == 0)
                  & (lax.broadcasted_iota(jnp.int32, (8, 128), 1) == 0))
    count_ref[0] = jnp.sum(jnp.where(first_only, C[0] + C[1], 0.0)).astype(jnp.int32)
    for c in pending:
        c.wait_send()


def per_device(tokens, w_gate, w_up, w_down, router_logits, expert_ids, draft_lengths, accept_mask):
    nx, ny = lax.axis_size("ep") // 2, lax.axis_size("tp")
    rows, width = tokens.shape
    hid = w_gate.shape[2]
    ncol = width // ny
    chunks = ny
    kc = width // chunks
    half = rows // 2
    cfg = dict(nx=nx, ny=ny, chunks=chunks, rows=rows, kc=kc, ncol=ncol, hid=hid, nexp=lax.axis_size("ep"))
    hx, hy = nx // 2, ny // 2
    dma = pltpu.SemaphoreType.DMA
    scratch = [
        pltpu.VMEM((chunks, nx, rows, kc), BF16),
        pltpu.VMEM((nx, rows, 128), BF16),
        pltpu.VMEM((2, width, hid), BF16),
        pltpu.VMEM((2, width, hid), BF16),
        pltpu.VMEM((ny, 2 * hid, ncol), BF16),
        pltpu.VMEM((2, 2, nx * rows, hid), F32),
        pltpu.VMEM((ny, nx, half, ncol), BF16),
        pltpu.VMEM((ny, nx, half, ncol), BF16),
        pltpu.VMEM((2, hx, ny, half, ncol), BF16),
        pltpu.VMEM((2, hy, nx, half, ncol), BF16),
        pltpu.VMEM((ny, half, ncol), BF16),
        pltpu.VMEM((nx, half, ncol), BF16),
        pltpu.VMEM((2, 8, 128), F32),
        dma((chunks,)), dma((chunks, 2)), dma((chunks, 2)), dma((chunks, 2)),
        dma((chunks + 1, hx, 2)), dma((chunks + 1, hx, 2)),
        dma((ny // 2, hx, 2)), dma((ny // 2, hx, 2)), dma((nx // 2, hy, 2)), dma((nx // 2, hy, 2)),
        dma((ny,)), dma((ny,)), dma((nx,)), dma((nx,)), dma(()), dma(()), dma((ny,)), dma((ny,)), dma((ny,)),
    ]
    anyspec = pl.BlockSpec(memory_space=pl.ANY)
    vmem = pl.BlockSpec(memory_space=pltpu.VMEM)
    smem = pl.BlockSpec(memory_space=pltpu.SMEM)
    mixed, accepted = pl.pallas_call(
        functools.partial(kernel, cfg),
        out_shape=(jax.ShapeDtypeStruct((rows, ncol), BF16), jax.ShapeDtypeStruct((1,), jnp.int32)),
        in_specs=[anyspec] * 4 + [vmem, vmem, smem, vmem],
        out_specs=(vmem, smem),
        scratch_shapes=scratch,
        name="routed_experts",
        compiler_params=pltpu.CompilerParams(collective_id=0, has_side_effects=True, vmem_limit_bytes=60 * 1024 * 1024),
    )(tokens, w_gate, w_up, w_down, router_logits.T, expert_ids.T, draft_lengths, accept_mask)
    return mixed, accepted


def solution(mesh):
    placed = (
        P(("groups", "ep"), None),
        P("ep", None, "tp"),
        P("ep", None, "tp"),
        P("ep", "tp", None),
        P(("groups", "ep"), None),
        P(("groups", "ep"), None),
        P(("groups", "ep")),
        P(("groups", "ep"), None),
    )
    return jax.shard_map(
        per_device,
        mesh=mesh,
        in_specs=placed,
        out_specs=(P(("groups", "ep"), "tp"), P("groups")),
        check_vma=False,
    )
```

```python
import functools

import jax
import jax.numpy as jnp
from jax import lax
from jax.experimental import pallas as pl
from jax.experimental.pallas import tpu as pltpu
from jax.sharding import PartitionSpec as P

MESH = pl.DeviceIdType.MESH
DRAFT = 8
SCALE = 2.827
BF16, F32 = jnp.bfloat16, jnp.float32


def signed_order(n):
    half = n // 2
    order = [half]
    for d in range(half - 1, 0, -1):
        order += [d, -d]
    return order + [0]


def gather_order(nx, ny, na, unit_a, unit_b, lat):
    hx, hy = nx // 2, ny // 2
    jobs = {}
    for st in range(hx):
        cut = 0.5 if st == hx - 1 else 1.0
        for d in range(2):
            for q in range(na):
                jobs["a", q, st, d] = (d, unit_a * cut, ("a", q, st - 1, d) if st else None, 100 + q)
            jobs["g", 0, st, d] = (d, unit_b * cut / 4, ("g", 0, st - 1, d) if st else None, 200)
            if st < hx - 1 or d == 0:
                jobs["b", 0, st, d] = (d, unit_b, ("b", 0, st - 1, d) if st else None, 0)
    for j in range(1, nx):
        dep = ("b", 0, j - 1, 0) if j <= hx else ("b", 0, nx - 1 - j, 1)
        for d in range(2):
            for st in range(hy):
                if st < hy - 1 or j % 2 != d:
                    jobs["y", j, st, d] = (2 + d, unit_b, dep if st == 0 else ("y", j, st - 1, d), -min(j, nx - j))
    ready = {k: 0.0 for k, v in jobs.items() if v[2] is None}
    free, order, arrive, left = [0.0] * 4, [], {}, set(jobs)
    while left:
        best = None
        for link in range(4):
            able = [k for k in left if jobs[k][0] == link and k in ready]
            if able:
                t = max(free[link], min(ready[k] for k in able))
                k = min((k for k in able if ready[k] <= t + 1e-9), key=lambda k: (jobs[k][3], ready[k], k))
                if best is None or t < best[0]:
                    best = (t, k)
        t, k = best
        free[jobs[k][0]] = t + jobs[k][1]
        arrive[k] = free[jobs[k][0]] + lat
        order.append((t, k))
        left.discard(k)
        for m, v in jobs.items():
            if v[2] == k:
                ready[m] = arrive[k]
    return sorted(order), {k: v[2] for k, v in jobs.items()}, arrive


def kernel(cfg, tok_ref, wg_ref, wu_ref, wd_ref, logit_ref, ids_ref, len_ref, mask_ref, out_ref, count_ref,
           XA, XB, G, W, WD, ACC, P1, P2, RB1, RB2, F1, F2, C,
           ta_sem, tb_sem, wla_sem, wlb_sem, wra_sem, wrb_sem, a_recv, b_recv, g_recv, y_recv, h1_recv, h2_recv,
           f1_recv, f2_recv, c_recv, d_sem, dr_recv, send_sem):
    NX, NY, NA = cfg["nx"], cfg["ny"], cfg["na"]
    HX, HY = NX // 2, NY // 2
    rows = cfg["rows"]
    half = rows // 2
    ka, kb = cfg["ka"], cfg["kb"]
    ncol = cfg["ncol"]
    hid = cfg["hid"]
    nexp = cfg["nexp"]
    n_ep = 2 * NX
    base = NA * ka
    ep = lax.axis_index("ep")
    tp = lax.axis_index("tp")
    core = lax.rem(ep, 2)
    partner = {"ep": ep + 1 - 2 * core}

    def xdev(d):
        return {"ep": lax.rem(ep + (2 * d) % n_ep, n_ep)}

    def ydev(d):
        return {"tp": lax.rem(tp + d % NY, NY)}

    def slice_of(r, size, start=0):
        return pl.ds(pl.multiple_of(start + lax.rem(tp + r % NY, NY) * size, 128), size)

    kk = signed_order(NY)
    A_SEND, B_SEND, G_SEND, Y_SEND, H1_SEND, H2_SEND, F1_SEND, F2_SEND, C_SEND, W_SEND, D_SEND = range(11)

    def remote(src, dst, send, recv, dev):
        c = pltpu.make_async_remote_copy(src_ref=src, dst_ref=dst, send_sem=send_sem.at[send], recv_sem=recv,
                                         device_id=dev, device_id_type=MESH)
        c.start()
        return c

    tok_a, tok_b = [], []
    for r in range(NY):
        c = pltpu.make_async_copy(tok_ref.at[:, slice_of(r, kb, base)], XB.at[r, 0], tb_sem.at[r])
        c.start()
        tok_b.append(c)
    for q in range(NA):
        c = pltpu.make_async_copy(tok_ref.at[:, pl.ds(q * ka, ka)], XA.at[q, 0], ta_sem.at[q])
        c.start()
        tok_a.append(c)
    rows_a = [pl.ds(q * ka, ka) for q in range(NA)]
    rows_b = [pl.ds(base + r * kb, kb) for r in range(NY)]
    from_b = [slice_of(r, kb, base) for r in range(NY)]
    for src, dst, sem in ([(rows_a[q], rows_a[q], wla_sem.at[q]) for q in range(NA)]
                          + [(from_b[r], rows_b[r], wlb_sem.at[r]) for r in range(NY)]):
        for i, w in enumerate((wg_ref, wu_ref)):
            pltpu.make_async_copy(w.at[0, src], W.at[0, i, dst], sem).start()
    dl = []
    dcols = []
    for p in range(NY):
        dcols.append(slice_of(kk[p], ncol))
        c = pltpu.make_async_copy(wd_ref.at[0, :, dcols[p]], WD.at[p, pl.ds(0, hid)], d_sem.at[p])
        c.start()
        dl.append(c)

    barrier = pltpu.get_barrier_semaphore()
    peers = [partner, xdev(1), xdev(-1), ydev(1), ydev(-1)]
    for dev in peers:
        pl.semaphore_signal(barrier, inc=1, device_id=dev, device_id_type=MESH)

    logits = logit_ref[...]
    sig = 1.0 / (1.0 + jnp.exp(-logits))
    gates = SCALE * sig / jnp.sum(sig, axis=0, keepdims=True)
    lane = lax.broadcasted_iota(jnp.int32, (1, rows), 1)
    length = jnp.zeros((1, rows), jnp.int32)
    for r in range(rows // DRAFT):
        length = jnp.where(lane // DRAFT == r, len_ref[r], length)
    gates = jnp.where(lane % DRAFT < length, gates, 0.0)
    mrow = lax.broadcasted_iota(jnp.int32, mask_ref.shape, 0)
    mcol = lax.broadcasted_iota(jnp.int32, mask_ref.shape, 1)
    mlen = jnp.zeros(mask_ref.shape, jnp.int32)
    for r in range(rows // DRAFT):
        mlen = jnp.where(mrow == r, len_ref[r], mlen)
    passed = jnp.where(mcol < mlen, mask_ref[...], 0).astype(F32)
    run = passed[:, 0:1]
    local_count = run
    for j in range(1, DRAFT):
        run = run * passed[:, j:j + 1]
        local_count = local_count + run
    local_count = jnp.sum(local_count, axis=0, keepdims=True)
    feat = lax.broadcasted_iota(jnp.int32, (128, rows), 0)
    dense = jnp.zeros((128, rows), F32)
    ids = ids_ref[...]
    for k in range(ids.shape[0]):
        e = ids[k:k + 1, :]
        dense = dense + jnp.where((feat == e) | (feat == e + nexp), gates[k:k + 1, :], 0.0)
    high = dense.astype(BF16)
    packed = jnp.where(feat < nexp, high.astype(F32), dense - high.astype(F32))
    packed = packed + jnp.where(feat == 2 * nexp, local_count, 0.0)
    eye = (lax.broadcasted_iota(jnp.int32, (rows, rows), 0) == lax.broadcasted_iota(jnp.int32, (rows, rows), 1))
    turned = lax.dot_general(eye.astype(F32).astype(BF16), packed.astype(BF16), (((1,), (1,)), ((), ())),
                             preferred_element_type=F32)
    G[0] = turned.astype(BF16)

    pl.semaphore_wait(barrier, len(peers))

    lo, hi = pl.ds(0, half), pl.ds(half, half)
    order, deps, arrive = gather_order(NX, NY, NA, cfg["ta"], cfg["tb"], cfg["lat"])
    copies = {}
    heard = set()

    def hear(key):
        if key not in heard:
            heard.add(key)
            copies[key].wait_recv()

    def own_ready(kind, n):
        if (kind, n) not in heard:
            heard.add((kind, n))
            (tok_a if kind == "a" else tok_b)[n].wait()

    def send(key):
        kind, n, st, d = key
        if deps[key] is not None:
            hear(deps[key])
        last = st == HX - 1
        if kind == "y":
            r = (NY - st) % NY if d == 0 else st
            to = NY - 1 - st if d == 0 else st + 1
            copies[key] = remote(XB.at[r, n], XB.at[to, n], Y_SEND, y_recv.at[n, st, d], ydev(1 if d == 0 else -1))
            return
        a, b = (st, st + 1) if d == 0 else ((NX - st) % NX, NX - st - 1)
        dev = xdev(1 if d == 0 else -1)
        if kind == "b":
            own_ready("b", 0)
            copies[key] = remote(XB.at[0, a], XB.at[0, b], B_SEND, b_recv.at[st, d], dev)
            return
        ref, sem, recv = (XA.at[n], A_SEND, a_recv.at[n, st, d]) if kind == "a" else (G, G_SEND, g_recv.at[st, d])
        if kind == "a":
            own_ready("a", n)
        src, dst = ref.at[a], ref.at[b]
        if last:
            part = lo if d == 0 else hi
            src, dst = src.at[part], dst.at[part]
        copies[key] = remote(src, dst, sem, recv, dev)

    started = []

    def gate_up(x, part, sem_l, sem_r):
        for e in range(2):
            both = W.at[e, :, part]
            pltpu.make_async_copy(both, both, sem_l if e == 0 else sem_r).wait()
            for i in range(2):
                y = jnp.dot(x, W[e, i, part, :], preferred_element_type=F32)
                ACC[i, e] = ACC[i, e] + y if started else y
        started.append(1)

    def gate_up_a(q):
        for d in range(2):
            for st in range(HX):
                hear(("a", q, st, d))
        gate_up(XA[q].reshape(NX * rows, ka), rows_a[q], wla_sem.at[q], wra_sem.at[q])

    def keys_b(r):
        keys = []
        for j in range(1, NX):
            for d in range(2):
                st = NY - 1 - r if d == 0 else r - 1
                if ("y", j, st, d) in deps:
                    keys.append(("y", j, st, d))
            if r == 0:
                keys.append(("b", 0, j - 1, 0) if j <= HX else ("b", 0, NX - 1 - j, 1))
        return keys

    def gate_up_b(r):
        own_ready("b", r)
        for key in keys_b(r):
            hear(key)
        gate_up(XB[r].reshape(NX * rows, kb), rows_b[r], wlb_sem.at[r], wrb_sem.at[r])

    work = []
    for q in range(NA):
        work.append((max(arrive["a", q, st, d] for st in range(HX) for d in range(2)), "ga", q))
    for r in range(NY):
        work.append((max(arrive[key] for key in keys_b(r)), "gb", r))
    events = sorted([(t, 0, key) for t, key in order] + [(t, 1, (kind, n)) for t, kind, n in work])
    sent = 0
    dr = []
    for t, which, key in events:
        if which == 0:
            send(key)
            sent += 1
        elif key[0] == "ga":
            gate_up_a(key[1])
        else:
            gate_up_b(key[1])
        if sent == 4 and not dr:
            def push(src, dst, sem):
                for i, w in enumerate((wg_ref, wu_ref)):
                    remote(w.at[0, src], W.at[1, i, dst], W_SEND, sem, partner)

            for _, kind, n in sorted(work):
                if kind == "ga":
                    push(rows_a[n], rows_a[n], wra_sem.at[n])
                else:
                    push(from_b[n], rows_b[n], wrb_sem.at[n])
            for p in range(NY):
                dr.append(remote(wd_ref.at[0, :, dcols[p]], WD.at[p, pl.ds(hid, hid)], D_SEND, dr_recv.at[p], partner))
    for d in range(2):
        for st in range(HX):
            hear(("g", 0, st, d))

    g_all = G[...].reshape(NX * rows, 128).astype(F32)
    glane = lax.broadcasted_iota(jnp.int32, (NX * rows, 128), 1)
    grow = lax.broadcasted_iota(jnp.int32, (NX * rows, 128), 0)
    tally = jnp.where((glane == 2 * nexp) & (grow % rows == 0), g_all, 0.0)
    C[0] = jnp.zeros((8, 128), F32) + jnp.sum(tally)
    c_copy = remote(C.at[0], C.at[1], C_SEND, c_recv, partner)
    hs = []
    for e in range(2):
        expert = ep if e == 0 else partner["ep"]
        gate = jnp.sum(jnp.where((glane == expert) | (glane == expert + nexp), g_all, 0.0), axis=1, keepdims=True)
        g, u = ACC[0, e], ACC[1, e]
        hs.append((gate * (g / (1.0 + jnp.exp(-g)) * u)).astype(BF16))
    h = jnp.concatenate(hs, axis=1)

    def down(p):
        dl[p].wait()
        dr[p].wait_recv()
        y = jnp.dot(h, WD[p], preferred_element_type=F32).astype(BF16).reshape(NX, rows, ncol)
        P1[p] = y[:, :half]
        P2[p] = y[:, half:]

    pos = {k: p for p, k in enumerate(kk)}
    NQ = NY // 2
    NJ = NX // 2
    h1, h2 = {}, {}

    def add(dst, src):
        dst[...] = (dst[...].astype(F32) + src[...].astype(F32)).astype(BF16)

    def h1_step(q, s):
        for d in range(2):
            slot = (HX + s) % NX if d == 0 else HX - s
            if s == 0:
                p, n = 2 * q + d, 1
            else:
                p, n = 2 * q, 2
                h1[q, s - 1, d].wait_recv()
                pa, na = (2 * q + d, 1) if s == 1 else (p, n)
                add(P1.at[pl.ds(pa, na), slot], RB1.at[d, s - 1, pl.ds(pa, na)])
            h1[q, s, d] = remote(P1.at[pl.ds(p, n), slot], RB1.at[d, s, pl.ds(p, n)],
                                 H1_SEND, h1_recv.at[q, s, d], xdev(1 if d == 0 else -1))

    def h2_step(j, s):
        for d in range(2):
            p = pos[HY - s] if (d == 0 or s == 0) else pos[s - HY]
            mine = (j < NJ // 2) == (d == 0)
            rng = pl.ds(2 * j, 2)
            if s == 0 and not mine:
                continue
            if s > 0 and (s > 1 or mine):
                h2[j, s - 1, d].wait_recv()
                add(P2.at[p, rng], RB2.at[d, s - 1, rng])
            h2[j, s, d] = remote(P2.at[p, rng], RB2.at[d, s, rng],
                                 H2_SEND, h2_recv.at[j, s, d], ydev(1 if d == 0 else -1))

    down(0)
    for j in range(NJ):
        h2_step(j, 0)
    down(1)
    h1_step(0, 0)
    for q in range(1, NQ):
        down(2 * q)
        down(2 * q + 1)
        h1_step(q, 0)
        if q == 1:
            for j in range(NJ):
                h2_step(j, 1)
    for s in range(1, HX):
        for i in range(max(NQ, NJ)):
            if i < NQ:
                h1_step(i, s)
            if i < NJ and s + 1 < HY:
                h2_step(i, s + 1)

    f1, f2 = [], []
    last = NY - 1

    def h1_final(q):
        h1[q, HX - 1, 0].wait_recv()
        h1[q, HX - 1, 1].wait_recv()
        r = pl.ds(2 * q, 2)
        P1[r, 0] = (P1[r, 0].astype(F32) + RB1[0, HX - 1, r].astype(F32) + RB1[1, HX - 1, r].astype(F32)).astype(BF16)
        for p in (2 * q, 2 * q + 1):
            if kk[p] != 0:
                f1.append(remote(P1.at[p, 0], F1.at[p], F1_SEND, f1_recv.at[p], ydev(kk[p])))

    def h2_final(j):
        h2[j, HY - 1, 0].wait_recv()
        h2[j, HY - 1, 1].wait_recv()
        r = pl.ds(2 * j, 2)
        P2[last, r] = (P2[last, r].astype(F32) + RB2[0, HY - 1, r].astype(F32) + RB2[1, HY - 1, r].astype(F32)).astype(BF16)
        for slot in (2 * j, 2 * j + 1):
            if slot != 0:
                f2.append(remote(P2.at[last, slot], F2.at[slot], F2_SEND, f2_recv.at[slot], xdev(-slot)))

    for i in range(max(NQ, NJ)):
        if i < NJ:
            h2_final(i)
        if i < NQ:
            h1_final(i)

    for c in f1 + f2:
        c.wait_recv()
    a = P1[last, 0].astype(F32)
    for p in range(NY):
        if kk[p] != 0:
            a = a + F1[p].astype(F32)
    out_ref[pl.ds(0, half), :] = a.astype(BF16)
    b = P2[last, 0].astype(F32)
    for slot in range(1, NX):
        b = b + F2[slot].astype(F32)
    out_ref[pl.ds(half, half), :] = b.astype(BF16)
    c_copy.wait_recv()
    first_only = ((lax.broadcasted_iota(jnp.int32, (8, 128), 0) == 0)
                  & (lax.broadcasted_iota(jnp.int32, (8, 128), 1) == 0))
    count_ref[0] = jnp.sum(jnp.where(first_only, C[0] + C[1], 0.0)).astype(jnp.int32)

    def drained(sem, ref):
        pltpu.make_async_copy(ref, ref, send_sem.at[sem]).wait()

    most = pl.ds(0, NX - 1)
    drained(A_SEND, XA.at[:, most])
    drained(B_SEND, XB.at[0, most])
    drained(G_SEND, G.at[most])
    drained(Y_SEND, XB.at[pl.ds(0, NY - 1), most])
    drained(W_SEND, W.at[1])
    drained(D_SEND, WD.at[:, pl.ds(0, hid)])
    drained(C_SEND, C.at[0])
    drained(H1_SEND, P1.at[:, most])
    drained(H2_SEND, P2.at[pl.ds(0, NY - 1)])
    drained(F1_SEND, F1.at[pl.ds(0, NY - 1)])
    drained(F2_SEND, F2.at[most])


def per_device(tokens, w_gate, w_up, w_down, router_logits, expert_ids, draft_lengths, accept_mask):
    nx, ny = lax.axis_size("ep") // 2, lax.axis_size("tp")
    rows, width = tokens.shape
    hid = w_gate.shape[2]
    ncol = width // ny
    half = rows // 2
    hx, hy = nx // 2, ny // 2
    kb = 512
    na = 3
    ka = (width - ny * kb) // na
    us_per_col = rows * 2 / 46.6e3
    cfg = dict(nx=nx, ny=ny, na=na, ka=ka, kb=kb, rows=rows, ncol=ncol, hid=hid, nexp=lax.axis_size("ep"),
               ta=ka * us_per_col, tb=kb * us_per_col, lat=2.0)
    dma = pltpu.SemaphoreType.DMA
    scratch = [
        pltpu.VMEM((na, nx, rows, ka), BF16),
        pltpu.VMEM((ny, nx, rows, kb), BF16),
        pltpu.VMEM((nx, rows, 128), BF16),
        pltpu.VMEM((2, 2, width, hid), BF16),
        pltpu.VMEM((ny, 2 * hid, ncol), BF16),
        pltpu.VMEM((2, 2, nx * rows, hid), F32),
        pltpu.VMEM((ny, nx, half, ncol), BF16),
        pltpu.VMEM((ny, nx, half, ncol), BF16),
        pltpu.VMEM((2, hx, ny, half, ncol), BF16),
        pltpu.VMEM((2, hy, nx, half, ncol), BF16),
        pltpu.VMEM((ny, half, ncol), BF16),
        pltpu.VMEM((nx, half, ncol), BF16),
        pltpu.VMEM((2, 8, 128), F32),
        dma((na,)), dma((ny,)), dma((na,)), dma((ny,)), dma((na,)), dma((ny,)),
        dma((na, hx, 2)), dma((hx, 2)), dma((hx, 2)), dma((nx, hy, 2)), dma((ny // 2, hx, 2)), dma((nx // 2, hy, 2)),
        dma((ny,)), dma((nx,)), dma(()), dma((ny,)), dma((ny,)), dma((11,)),
    ]
    anyspec = pl.BlockSpec(memory_space=pl.ANY)
    vmem = pl.BlockSpec(memory_space=pltpu.VMEM)
    smem = pl.BlockSpec(memory_space=pltpu.SMEM)
    mixed, accepted = pl.pallas_call(
        functools.partial(kernel, cfg),
        out_shape=(jax.ShapeDtypeStruct((rows, ncol), BF16), jax.ShapeDtypeStruct((1,), jnp.int32)),
        in_specs=[anyspec] * 4 + [vmem, vmem, smem, vmem],
        out_specs=(vmem, smem),
        scratch_shapes=scratch,
        name="routed_experts",
        compiler_params=pltpu.CompilerParams(collective_id=0, has_side_effects=True, vmem_limit_bytes=60 * 1024 * 1024),
    )(tokens, w_gate, w_up, w_down, router_logits.T, expert_ids.T, draft_lengths, accept_mask)
    return mixed, accepted


def solution(mesh):
    placed = (
        P(("groups", "ep"), None),
        P("ep", None, "tp"),
        P("ep", None, "tp"),
        P("ep", "tp", None),
        P(("groups", "ep"), None),
        P(("groups", "ep"), None),
        P(("groups", "ep")),
        P(("groups", "ep"), None),
    )
    return jax.shard_map(
        per_device,
        mesh=mesh,
        in_specs=placed,
        out_specs=(P(("groups", "ep"), "tp"), P("groups")),
        check_vma=False,
    )
```

```python
import functools

import jax
import jax.numpy as jnp
from jax import lax
from jax.experimental import pallas as pl
from jax.experimental.pallas import tpu as pltpu
from jax.sharding import PartitionSpec as P

MESH = pl.DeviceIdType.MESH
DRAFT = 8
SCALE = 2.827
BF16, F32 = jnp.bfloat16, jnp.float32


def signed_order(n):
    half = n // 2
    order = [half]
    for d in range(half - 1, 0, -1):
        order += [d, -d]
    return order + [0]


def gather_order(nx, ny, na, unit_a, unit_b, lat):
    hx, hy = nx // 2, ny // 2
    jobs = {}
    for st in range(hx):
        cut = 0.5 if st == hx - 1 else 1.0
        for d in range(2):
            for q in range(na):
                jobs["a", q, st, d] = (d, unit_a * cut, ("a", q, st - 1, d) if st else None, 100 + q)
            jobs["g", 0, st, d] = (d, unit_b * cut / 4, ("g", 0, st - 1, d) if st else None, 200)
            if st < hx - 1 or d == 0:
                jobs["b", 0, st, d] = (d, unit_b, ("b", 0, st - 1, d) if st else None, 0)
    for j in range(1, nx):
        dep = ("b", 0, j - 1, 0) if j <= hx else ("b", 0, nx - 1 - j, 1)
        for d in range(2):
            for st in range(hy):
                if st < hy - 1 or j % 2 != d:
                    jobs["y", j, st, d] = (2 + d, unit_b, dep if st == 0 else ("y", j, st - 1, d), -min(j, nx - j))
    ready = {k: 0.0 for k, v in jobs.items() if v[2] is None}
    free, order, arrive, left = [0.0] * 4, [], {}, set(jobs)
    while left:
        best = None
        for link in range(4):
            able = [k for k in left if jobs[k][0] == link and k in ready]
            if able:
                t = max(free[link], min(ready[k] for k in able))
                k = min((k for k in able if ready[k] <= t + 1e-9), key=lambda k: (jobs[k][3], ready[k], k))
                if best is None or t < best[0]:
                    best = (t, k)
        t, k = best
        free[jobs[k][0]] = t + jobs[k][1]
        arrive[k] = free[jobs[k][0]] + lat
        order.append((t, k))
        left.discard(k)
        for m, v in jobs.items():
            if v[2] == k:
                ready[m] = arrive[k]
    return sorted(order), {k: v[2] for k, v in jobs.items()}, arrive


def kernel(cfg, tok_ref, wg_ref, wu_ref, wd_ref, logit_ref, ids_ref, len_ref, mask_ref, out_ref, count_ref,
           XA, XB, G, W, WD, ACC, P1, P2, RB1, RB2, F1, F2, C,
           ta_sem, tb_sem, wla_sem, wlb_sem, wra_sem, wrb_sem, a_recv, b_recv, g_recv, y_recv, h1_recv, h2_recv,
           f1_recv, f2_recv, c_recv, d_sem, dr_recv, send_sem):
    NX, NY, NA = cfg["nx"], cfg["ny"], cfg["na"]
    HX, HY = NX // 2, NY // 2
    rows = cfg["rows"]
    half = rows // 2
    ka, kb = cfg["ka"], cfg["kb"]
    ncol = cfg["ncol"]
    hid = cfg["hid"]
    nexp = cfg["nexp"]
    n_ep = 2 * NX
    base = NA * ka
    ep = lax.axis_index("ep")
    tp = lax.axis_index("tp")
    core = lax.rem(ep, 2)
    partner = {"ep": ep + 1 - 2 * core}

    def xdev(d):
        return {"ep": lax.rem(ep + (2 * d) % n_ep, n_ep)}

    def ydev(d):
        return {"tp": lax.rem(tp + d % NY, NY)}

    def slice_of(r, size, start=0):
        return pl.ds(pl.multiple_of(start + lax.rem(tp + r % NY, NY) * size, 128), size)

    kk = signed_order(NY)
    A_SEND, B_SEND, G_SEND, Y_SEND, H1_SEND, H2_SEND, F1_SEND, F2_SEND, C_SEND, W_SEND, D_SEND = range(11)

    def remote(src, dst, send, recv, dev):
        c = pltpu.make_async_remote_copy(src_ref=src, dst_ref=dst, send_sem=send_sem.at[send], recv_sem=recv,
                                         device_id=dev, device_id_type=MESH)
        c.start()
        return c

    tok_a, tok_b = [], []
    for r in range(NY):
        c = pltpu.make_async_copy(tok_ref.at[:, slice_of(r, kb, base)], XB.at[r, 0], tb_sem.at[r])
        c.start()
        tok_b.append(c)
    for q in range(NA):
        c = pltpu.make_async_copy(tok_ref.at[:, pl.ds(q * ka, ka)], XA.at[q, 0], ta_sem.at[q])
        c.start()
        tok_a.append(c)
    rows_a = [pl.ds(q * ka, ka) for q in range(NA)]
    rows_b = [pl.ds(base + r * kb, kb) for r in range(NY)]
    from_b = [slice_of(r, kb, base) for r in range(NY)]
    for src, dst, sem in ([(rows_a[q], rows_a[q], wla_sem.at[q]) for q in range(NA)]
                          + [(from_b[r], rows_b[r], wlb_sem.at[r]) for r in range(NY)]):
        for i, w in enumerate((wg_ref, wu_ref)):
            pltpu.make_async_copy(w.at[0, src], W.at[0, i, dst], sem).start()
    dl = []
    dcols = []
    for p in range(NY):
        dcols.append(slice_of(kk[p], ncol))
        c = pltpu.make_async_copy(wd_ref.at[0, :, dcols[p]], WD.at[p, pl.ds(0, hid)], d_sem.at[p])
        c.start()
        dl.append(c)

    barrier = pltpu.get_barrier_semaphore()
    peers = [partner, xdev(1), xdev(-1), ydev(1), ydev(-1)]
    for dev in peers:
        pl.semaphore_signal(barrier, inc=1, device_id=dev, device_id_type=MESH)

    logits = logit_ref[...]
    sig = 1.0 / (1.0 + jnp.exp(-logits))
    gates = SCALE * sig / jnp.sum(sig, axis=0, keepdims=True)
    lane = lax.broadcasted_iota(jnp.int32, (1, rows), 1)
    length = jnp.zeros((1, rows), jnp.int32)
    for r in range(rows // DRAFT):
        length = jnp.where(lane // DRAFT == r, len_ref[r], length)
    gates = jnp.where(lane % DRAFT < length, gates, 0.0)
    mrow = lax.broadcasted_iota(jnp.int32, mask_ref.shape, 0)
    mcol = lax.broadcasted_iota(jnp.int32, mask_ref.shape, 1)
    mlen = jnp.zeros(mask_ref.shape, jnp.int32)
    for r in range(rows // DRAFT):
        mlen = jnp.where(mrow == r, len_ref[r], mlen)
    passed = jnp.where(mcol < mlen, mask_ref[...], 0).astype(F32)
    run = passed[:, 0:1]
    local_count = run
    for j in range(1, DRAFT):
        run = run * passed[:, j:j + 1]
        local_count = local_count + run
    local_count = jnp.sum(local_count, axis=0, keepdims=True)
    feat = lax.broadcasted_iota(jnp.int32, (128, rows), 0)
    dense = jnp.zeros((128, rows), F32)
    ids = ids_ref[...]
    for k in range(ids.shape[0]):
        e = ids[k:k + 1, :]
        dense = dense + jnp.where((feat == e) | (feat == e + nexp), gates[k:k + 1, :], 0.0)
    high = dense.astype(BF16)
    packed = jnp.where(feat < nexp, high.astype(F32), dense - high.astype(F32))
    packed = packed + jnp.where(feat == 2 * nexp, local_count, 0.0)
    eye = (lax.broadcasted_iota(jnp.int32, (rows, rows), 0) == lax.broadcasted_iota(jnp.int32, (rows, rows), 1))
    turned = lax.dot_general(eye.astype(F32).astype(BF16), packed.astype(BF16), (((1,), (1,)), ((), ())),
                             preferred_element_type=F32)
    G[0] = turned.astype(BF16)

    pl.semaphore_wait(barrier, len(peers))

    lo, hi = pl.ds(0, half), pl.ds(half, half)
    order, deps, arrive = gather_order(NX, NY, NA, cfg["ta"], cfg["tb"], cfg["lat"])
    copies = {}
    heard = set()

    def hear(key):
        if key not in heard:
            heard.add(key)
            copies[key].wait_recv()

    def own_ready(kind, n):
        if (kind, n) not in heard:
            heard.add((kind, n))
            (tok_a if kind == "a" else tok_b)[n].wait()

    def send(key):
        kind, n, st, d = key
        if deps[key] is not None:
            hear(deps[key])
        last = st == HX - 1
        if kind == "y":
            r = (NY - st) % NY if d == 0 else st
            to = NY - 1 - st if d == 0 else st + 1
            copies[key] = remote(XB.at[r, n], XB.at[to, n], Y_SEND, y_recv.at[n, st, d], ydev(1 if d == 0 else -1))
            return
        a, b = (st, st + 1) if d == 0 else ((NX - st) % NX, NX - st - 1)
        dev = xdev(1 if d == 0 else -1)
        if kind == "b":
            own_ready("b", 0)
            copies[key] = remote(XB.at[0, a], XB.at[0, b], B_SEND, b_recv.at[st, d], dev)
            return
        ref, sem, recv = (XA.at[n], A_SEND, a_recv.at[n, st, d]) if kind == "a" else (G, G_SEND, g_recv.at[st, d])
        if kind == "a":
            own_ready("a", n)
        src, dst = ref.at[a], ref.at[b]
        if last:
            part = lo if d == 0 else hi
            src, dst = src.at[part], dst.at[part]
        copies[key] = remote(src, dst, sem, recv, dev)

    started = []

    def gate_up(x, part, sem_l, sem_r):
        for e in range(2):
            both = W.at[e, :, part]
            pltpu.make_async_copy(both, both, sem_l if e == 0 else sem_r).wait()
            for i in range(2):
                y = jnp.dot(x, W[e, i, part, :], preferred_element_type=F32)
                ACC[i, e] = ACC[i, e] + y if started else y
        started.append(1)

    def gate_up_a(q):
        for d in range(2):
            for st in range(HX):
                hear(("a", q, st, d))
        gate_up(XA[q].reshape(NX * rows, ka), rows_a[q], wla_sem.at[q], wra_sem.at[q])

    def keys_b(r):
        keys = []
        for j in range(1, NX):
            for d in range(2):
                st = NY - 1 - r if d == 0 else r - 1
                if ("y", j, st, d) in deps:
                    keys.append(("y", j, st, d))
            if r == 0:
                keys.append(("b", 0, j - 1, 0) if j <= HX else ("b", 0, NX - 1 - j, 1))
        return keys

    def gate_up_b(r):
        own_ready("b", r)
        for key in keys_b(r):
            hear(key)
        gate_up(XB[r].reshape(NX * rows, kb), rows_b[r], wlb_sem.at[r], wrb_sem.at[r])

    work = []
    for q in range(NA):
        work.append((max(arrive["a", q, st, d] for st in range(HX) for d in range(2)), "ga", q))
    for r in range(NY):
        work.append((max(arrive[key] for key in keys_b(r)), "gb", r))
    pushes, clock = [], 0.0
    for need, kind, n in sorted(work):
        for i in range(2):
            pushes.append((min(clock, need - 3.0), "w", (kind, n, i)))
            clock += (ka if kind == "ga" else kb) * hid * 2 / cfg["push_rate"]
    for p in range(NY):
        pushes.append((clock, "d", p))
        clock += ncol * hid * 2 / cfg["push_rate"]
    dr = []

    def push(kind, what):
        if kind == "d":
            dr.append(remote(wd_ref.at[0, :, dcols[what]], WD.at[what, pl.ds(hid, hid)], D_SEND, dr_recv.at[what], partner))
            return
        group, n, i = what
        src, dst, sem = (rows_a[n], rows_a[n], wra_sem.at[n]) if group == "ga" else (from_b[n], rows_b[n], wrb_sem.at[n])
        remote((wg_ref, wu_ref)[i].at[0, src], W.at[1, i, dst], W_SEND, sem, partner)

    events = sorted([(t, 1, n, ("s", key)) for n, (t, key) in enumerate(order)]
                    + [(t, 2, n, (kind, what)) for n, (t, kind, what) in enumerate(work)]
                    + [(t, 0, n, (kind, what)) for n, (t, kind, what) in enumerate(pushes)])
    for _, _, _, (kind, what) in events:
        if kind == "s":
            send(what)
        elif kind == "ga":
            gate_up_a(what)
        elif kind == "gb":
            gate_up_b(what)
        else:
            push(kind, what)
    for d in range(2):
        for st in range(HX):
            hear(("g", 0, st, d))

    g_all = G[...].reshape(NX * rows, 128).astype(F32)
    glane = lax.broadcasted_iota(jnp.int32, (NX * rows, 128), 1)
    grow = lax.broadcasted_iota(jnp.int32, (NX * rows, 128), 0)
    tally = jnp.where((glane == 2 * nexp) & (grow % rows == 0), g_all, 0.0)
    C[0] = jnp.zeros((8, 128), F32) + jnp.sum(tally)
    c_copy = remote(C.at[0], C.at[1], C_SEND, c_recv, partner)
    hs = []
    for e in range(2):
        expert = ep if e == 0 else partner["ep"]
        gate = jnp.sum(jnp.where((glane == expert) | (glane == expert + nexp), g_all, 0.0), axis=1, keepdims=True)
        g, u = ACC[0, e], ACC[1, e]
        hs.append((gate * (g / (1.0 + jnp.exp(-g)) * u)).astype(BF16))
    h = jnp.concatenate(hs, axis=1)

    def down(p):
        dl[p].wait()
        dr[p].wait_recv()
        y = jnp.dot(h, WD[p], preferred_element_type=F32).astype(BF16).reshape(NX, rows, ncol)
        P1[p] = y[:, :half]
        P2[p] = y[:, half:]

    pos = {k: p for p, k in enumerate(kk)}
    NQ = NY // 2
    NJ = NX // 2
    h1, h2 = {}, {}

    def add(dst, src):
        dst[...] = (dst[...].astype(F32) + src[...].astype(F32)).astype(BF16)

    def h1_step(q, s):
        for d in range(2):
            slot = (HX + s) % NX if d == 0 else HX - s
            if s == 0:
                p, n = 2 * q + d, 1
            else:
                p, n = 2 * q, 2
                h1[q, s - 1, d].wait_recv()
                pa, na = (2 * q + d, 1) if s == 1 else (p, n)
                add(P1.at[pl.ds(pa, na), slot], RB1.at[d, s - 1, pl.ds(pa, na)])
            h1[q, s, d] = remote(P1.at[pl.ds(p, n), slot], RB1.at[d, s, pl.ds(p, n)],
                                 H1_SEND, h1_recv.at[q, s, d], xdev(1 if d == 0 else -1))

    def h2_step(j, s):
        for d in range(2):
            p = pos[HY - s] if (d == 0 or s == 0) else pos[s - HY]
            mine = (j < NJ // 2) == (d == 0)
            rng = pl.ds(2 * j, 2)
            if s == 0 and not mine:
                continue
            if s > 0 and (s > 1 or mine):
                h2[j, s - 1, d].wait_recv()
                add(P2.at[p, rng], RB2.at[d, s - 1, rng])
            h2[j, s, d] = remote(P2.at[p, rng], RB2.at[d, s, rng],
                                 H2_SEND, h2_recv.at[j, s, d], ydev(1 if d == 0 else -1))

    down(0)
    for j in range(NJ):
        h2_step(j, 0)
    down(1)
    h1_step(0, 0)
    for q in range(1, NQ):
        down(2 * q)
        down(2 * q + 1)
        h1_step(q, 0)
        if q == 1:
            for j in range(NJ):
                h2_step(j, 1)
    for s in range(1, HX):
        for i in range(max(NQ, NJ)):
            if i < NQ:
                h1_step(i, s)
            if i < NJ and s + 1 < HY:
                h2_step(i, s + 1)

    f1, f2 = [], []
    last = NY - 1

    def h1_final(q):
        h1[q, HX - 1, 0].wait_recv()
        h1[q, HX - 1, 1].wait_recv()
        r = pl.ds(2 * q, 2)
        P1[r, 0] = (P1[r, 0].astype(F32) + RB1[0, HX - 1, r].astype(F32) + RB1[1, HX - 1, r].astype(F32)).astype(BF16)
        for p in (2 * q, 2 * q + 1):
            if kk[p] != 0:
                f1.append(remote(P1.at[p, 0], F1.at[p], F1_SEND, f1_recv.at[p], ydev(kk[p])))

    def h2_final(j):
        h2[j, HY - 1, 0].wait_recv()
        h2[j, HY - 1, 1].wait_recv()
        r = pl.ds(2 * j, 2)
        P2[last, r] = (P2[last, r].astype(F32) + RB2[0, HY - 1, r].astype(F32) + RB2[1, HY - 1, r].astype(F32)).astype(BF16)
        for slot in (2 * j, 2 * j + 1):
            if slot != 0:
                f2.append(remote(P2.at[last, slot], F2.at[slot], F2_SEND, f2_recv.at[slot], xdev(-slot)))

    for i in range(max(NQ, NJ)):
        if i < NJ:
            h2_final(i)
        if i < NQ:
            h1_final(i)

    for c in f1 + f2:
        c.wait_recv()
    a = P1[last, 0].astype(F32)
    for p in range(NY):
        if kk[p] != 0:
            a = a + F1[p].astype(F32)
    out_ref[pl.ds(0, half), :] = a.astype(BF16)
    b = P2[last, 0].astype(F32)
    for slot in range(1, NX):
        b = b + F2[slot].astype(F32)
    out_ref[pl.ds(half, half), :] = b.astype(BF16)
    c_copy.wait_recv()
    first_only = ((lax.broadcasted_iota(jnp.int32, (8, 128), 0) == 0)
                  & (lax.broadcasted_iota(jnp.int32, (8, 128), 1) == 0))
    count_ref[0] = jnp.sum(jnp.where(first_only, C[0] + C[1], 0.0)).astype(jnp.int32)

    def drained(sem, ref):
        pltpu.make_async_copy(ref, ref, send_sem.at[sem]).wait()

    most = pl.ds(0, NX - 1)
    drained(A_SEND, XA.at[:, most])
    drained(B_SEND, XB.at[0, most])
    drained(G_SEND, G.at[most])
    drained(Y_SEND, XB.at[pl.ds(0, NY - 1), most])
    drained(W_SEND, W.at[1])
    drained(D_SEND, WD.at[:, pl.ds(0, hid)])
    drained(C_SEND, C.at[0])
    drained(H1_SEND, P1.at[:, most])
    drained(H2_SEND, P2.at[pl.ds(0, NY - 1)])
    drained(F1_SEND, F1.at[pl.ds(0, NY - 1)])
    drained(F2_SEND, F2.at[most])


def per_device(tokens, w_gate, w_up, w_down, router_logits, expert_ids, draft_lengths, accept_mask):
    nx, ny = lax.axis_size("ep") // 2, lax.axis_size("tp")
    rows, width = tokens.shape
    hid = w_gate.shape[2]
    ncol = width // ny
    half = rows // 2
    hx, hy = nx // 2, ny // 2
    kb = 512
    na = 3
    ka = (width - ny * kb) // na
    us_per_col = rows * 2 / 46.6e3
    cfg = dict(nx=nx, ny=ny, na=na, ka=ka, kb=kb, rows=rows, ncol=ncol, hid=hid, nexp=lax.axis_size("ep"),
               ta=ka * us_per_col, tb=kb * us_per_col, lat=2.0,
               push_rate=450e3)
    dma = pltpu.SemaphoreType.DMA
    scratch = [
        pltpu.VMEM((na, nx, rows, ka), BF16),
        pltpu.VMEM((ny, nx, rows, kb), BF16),
        pltpu.VMEM((nx, rows, 128), BF16),
        pltpu.VMEM((2, 2, width, hid), BF16),
        pltpu.VMEM((ny, 2 * hid, ncol), BF16),
        pltpu.VMEM((2, 2, nx * rows, hid), F32),
        pltpu.VMEM((ny, nx, half, ncol), BF16),
        pltpu.VMEM((ny, nx, half, ncol), BF16),
        pltpu.VMEM((2, hx, ny, half, ncol), BF16),
        pltpu.VMEM((2, hy, nx, half, ncol), BF16),
        pltpu.VMEM((ny, half, ncol), BF16),
        pltpu.VMEM((nx, half, ncol), BF16),
        pltpu.VMEM((2, 8, 128), F32),
        dma((na,)), dma((ny,)), dma((na,)), dma((ny,)), dma((na,)), dma((ny,)),
        dma((na, hx, 2)), dma((hx, 2)), dma((hx, 2)), dma((nx, hy, 2)), dma((ny // 2, hx, 2)), dma((nx // 2, hy, 2)),
        dma((ny,)), dma((nx,)), dma(()), dma((ny,)), dma((ny,)), dma((11,)),
    ]
    anyspec = pl.BlockSpec(memory_space=pl.ANY)
    vmem = pl.BlockSpec(memory_space=pltpu.VMEM)
    smem = pl.BlockSpec(memory_space=pltpu.SMEM)
    mixed, accepted = pl.pallas_call(
        functools.partial(kernel, cfg),
        out_shape=(jax.ShapeDtypeStruct((rows, ncol), BF16), jax.ShapeDtypeStruct((1,), jnp.int32)),
        in_specs=[anyspec] * 4 + [vmem, vmem, smem, vmem],
        out_specs=(vmem, smem),
        scratch_shapes=scratch,
        name="routed_experts",
        compiler_params=pltpu.CompilerParams(collective_id=0, has_side_effects=True, vmem_limit_bytes=60 * 1024 * 1024),
    )(tokens, w_gate, w_up, w_down, router_logits.T, expert_ids.T, draft_lengths, accept_mask)
    return mixed, accepted


def solution(mesh):
    placed = (
        P(("groups", "ep"), None),
        P("ep", None, "tp"),
        P("ep", None, "tp"),
        P("ep", "tp", None),
        P(("groups", "ep"), None),
        P(("groups", "ep"), None),
        P(("groups", "ep")),
        P(("groups", "ep"), None),
    )
    return jax.shard_map(
        per_device,
        mesh=mesh,
        in_specs=placed,
        out_specs=(P(("groups", "ep"), "tp"), P("groups")),
        check_vma=False,
    )
```

```python
import functools

import jax
import jax.numpy as jnp
from jax import lax
from jax.experimental import pallas as pl
from jax.experimental.pallas import tpu as pltpu
from jax.sharding import PartitionSpec as P

MESH = pl.DeviceIdType.MESH
DRAFT = 8
SCALE = 2.827
BF16, F32 = jnp.bfloat16, jnp.float32


def signed_order(n):
    half = n // 2
    order = [half]
    for d in range(half - 1, 0, -1):
        order += [d, -d]
    return order + [0]


def gather_jobs(nx, na, ka, nb, nsub, kb, us_per_col, us_dot):
    hx = nx // 2
    jobs = {}
    for st in range(hx):
        cut = 0.5 if st == hx - 1 else 1.0
        for d in range(2):
            for q in range(na):
                jobs["a", q, st, d] = (d, ka * us_per_col * cut, [("a", q, st - 1, d)] if st else [], 100 + q)
            for n in range(nsub):
                jobs["b", n, st, d] = (d, kb / nsub * us_per_col * cut, [("b", n, st - 1, d)] if st else [], 0.1 * n)
            jobs["g", 0, st, d] = (d, 128 * us_per_col * cut, [("g", 0, st - 1, d)] if st else [], 1)
    for j in range(1, nx):
        for n in range(nsub):
            dep = [("b", n, st, d) for st, d in ((j - 1, 0), (nx - 1 - j, 1)) if st < hx]
            for d in range(2):
                far = min(j, nx - j)
                jobs["y", n, j, 0, d] = (2 + d, kb / nsub * us_per_col, dep, 10 - far)
                jobs["y", n, j, 1, d] = (2 + d, kb / nsub * us_per_col / 2, [("y", n, j, 0, d)], 9 - far)
    for q in range(na):
        jobs["ga", q] = (4, us_dot * ka, [("a", q, st, d) for st in range(hx) for d in range(2)], 500)
    slots, subs = range(1, nx), range(nsub)
    for r in range(nb):
        if r == 0:
            deps = [("b", n, st, d) for n in subs for st in range(hx) for d in range(2)]
        elif r == 2:
            deps = [("y", n, j, 1, d) for n in subs for j in slots for d in range(2)]
        else:
            deps = [("y", n, j, 0, 0 if r == 3 else 1) for n in subs for j in slots]
        jobs["gb", r] = (4, us_dot * kb, deps, 500)
    return jobs


def plan(jobs, lat):
    missing = {k: len(v[2]) for k, v in jobs.items()}
    users = {}
    for k, v in jobs.items():
        for dep in v[2]:
            users.setdefault(dep, []).append(k)
    resources = range(5)
    able = {r: [k for k in jobs if jobs[k][0] == r and not missing[k]] for r in resources}
    when = {k: 0.0 for k in jobs}
    free, order = [0.0 for _ in resources], []
    while len(order) < len(jobs):
        best = None
        for r in resources:
            if able[r]:
                t = max(free[r], min(when[k] for k in able[r]))
                k = min((k for k in able[r] if when[k] <= t + 1e-9), key=lambda k: (jobs[k][3], when[k], k))
                if best is None or t < best[0]:
                    best = (t, k)
        t, k = best
        r = jobs[k][0]
        able[r].remove(k)
        free[r] = t + jobs[k][1]
        order.append((t, k))
        for m in users.get(k, []):
            when[m] = max(when[m], free[r] + (0.0 if r == 4 else lat))
            missing[m] -= 1
            if not missing[m]:
                able[jobs[m][0]].append(m)
    return order


def kernel(cfg, tok_ref, wg_ref, wu_ref, wd_ref, logit_ref, ids_ref, len_ref, mask_ref, out_ref, count_ref,
           XA, XB, G, W, WD, ACC, P1, P2, RB1, RB2, F1, F2, C,
           ta_sem, tb_sem, wla_sem, wlb_sem, wra_sem, wrb_sem, a_recv, b_recv, g_recv, y_recv, h1_recv, h2_recv,
           f1_recv, f2_recv, c_recv, d_sem, dr_recv, send_sem):
    NX, NY, NA, NB, NSUB = cfg["nx"], cfg["ny"], cfg["na"], cfg["nb"], cfg["nsub"]
    HX, HY = NX // 2, NY // 2
    rows = cfg["rows"]
    half = rows // 2
    ka, kb = cfg["ka"], cfg["kb"]
    ncol = cfg["ncol"]
    hid = cfg["hid"]
    nexp = cfg["nexp"]
    n_ep = 2 * NX
    base = NA * ka
    ep = lax.axis_index("ep")
    tp = lax.axis_index("tp")
    core = lax.rem(ep, 2)
    partner = {"ep": ep + 1 - 2 * core}

    def xdev(d):
        return {"ep": lax.rem(ep + (2 * d) % n_ep, n_ep)}

    def ydev(d):
        return {"tp": lax.rem(tp + d % NY, NY)}

    def slice_of(r, count, size, start=0):
        return pl.ds(pl.multiple_of(start + lax.rem(tp + r % count, count) * size, 128), size)

    kk = signed_order(NY)
    A_SEND, B_SEND, G_SEND, Y_SEND, H1_SEND, H2_SEND, F1_SEND, F2_SEND, C_SEND, W_SEND, D_SEND = range(11)

    def remote(src, dst, send, recv, dev):
        c = pltpu.make_async_remote_copy(src_ref=src, dst_ref=dst, send_sem=send_sem.at[send], recv_sem=recv,
                                         device_id=dev, device_id_type=MESH)
        c.start()
        return c

    tok_a, tok_b = [], []
    for r in range(NB):
        c = pltpu.make_async_copy(tok_ref.at[:, slice_of(r, NB, kb, base)], XB.at[r, 0], tb_sem.at[r])
        c.start()
        tok_b.append(c)
    for q in range(NA):
        c = pltpu.make_async_copy(tok_ref.at[:, pl.ds(q * ka, ka)], XA.at[q, 0], ta_sem.at[q])
        c.start()
        tok_a.append(c)
    rows_a = [pl.ds(q * ka, ka) for q in range(NA)]
    rows_b = [pl.ds(base + r * kb, kb) for r in range(NB)]
    from_b = [slice_of(r, NB, kb, base) for r in range(NB)]
    for src, dst, sem in ([(rows_a[q], rows_a[q], wla_sem.at[q]) for q in range(NA)]
                          + [(from_b[r], rows_b[r], wlb_sem.at[r]) for r in range(NB)]):
        for i, w in enumerate((wg_ref, wu_ref)):
            pltpu.make_async_copy(w.at[0, src], W.at[0, i, dst], sem).start()
    dl = []
    dcols = []
    for p in range(NY):
        dcols.append(slice_of(kk[p], NY, ncol))
        c = pltpu.make_async_copy(wd_ref.at[0, :, dcols[p]], WD.at[p, pl.ds(0, hid)], d_sem.at[p])
        c.start()
        dl.append(c)

    barrier = pltpu.get_barrier_semaphore()
    peers = [partner, xdev(1), xdev(-1), ydev(1), ydev(-1)]
    for dev in peers:
        pl.semaphore_signal(barrier, inc=1, device_id=dev, device_id_type=MESH)

    logits = logit_ref[...]
    sig = 1.0 / (1.0 + jnp.exp(-logits))
    gates = SCALE * sig / jnp.sum(sig, axis=0, keepdims=True)
    lane = lax.broadcasted_iota(jnp.int32, (1, rows), 1)
    length = jnp.zeros((1, rows), jnp.int32)
    for r in range(rows // DRAFT):
        length = jnp.where(lane // DRAFT == r, len_ref[r], length)
    gates = jnp.where(lane % DRAFT < length, gates, 0.0)
    mrow = lax.broadcasted_iota(jnp.int32, mask_ref.shape, 0)
    mcol = lax.broadcasted_iota(jnp.int32, mask_ref.shape, 1)
    mlen = jnp.zeros(mask_ref.shape, jnp.int32)
    for r in range(rows // DRAFT):
        mlen = jnp.where(mrow == r, len_ref[r], mlen)
    passed = jnp.where(mcol < mlen, mask_ref[...], 0).astype(F32)
    run = passed[:, 0:1]
    local_count = run
    for j in range(1, DRAFT):
        run = run * passed[:, j:j + 1]
        local_count = local_count + run
    local_count = jnp.sum(local_count, axis=0, keepdims=True)
    feat = lax.broadcasted_iota(jnp.int32, (128, rows), 0)
    dense = jnp.zeros((128, rows), F32)
    ids = ids_ref[...]
    for k in range(ids.shape[0]):
        e = ids[k:k + 1, :]
        dense = dense + jnp.where((feat == e) | (feat == e + nexp), gates[k:k + 1, :], 0.0)
    high = dense.astype(BF16)
    packed = jnp.where(feat < nexp, high.astype(F32), dense - high.astype(F32))
    packed = packed + jnp.where(feat == 2 * nexp, local_count, 0.0)
    eye = (lax.broadcasted_iota(jnp.int32, (rows, rows), 0) == lax.broadcasted_iota(jnp.int32, (rows, rows), 1))
    turned = lax.dot_general(eye.astype(F32).astype(BF16), packed.astype(BF16), (((1,), (1,)), ((), ())),
                             preferred_element_type=F32)
    G[0] = turned.astype(BF16)

    pl.semaphore_wait(barrier, len(peers))

    lo, hi = pl.ds(0, half), pl.ds(half, half)
    jobs = gather_jobs(NX, NA, ka, NB, NSUB, kb, cfg["us_per_col"], cfg["us_dot"])
    order = plan(jobs, cfg["lat"])
    copies = {}
    heard = set()

    def hear(key):
        if key not in heard:
            heard.add(key)
            copies[key].wait_recv()

    def own_ready(kind, n):
        if (kind, n) not in heard:
            heard.add((kind, n))
            (tok_a if kind == "a" else tok_b)[n].wait()

    def send(key):
        kind, n, st, d = key[0], key[1], key[-2], key[-1]
        for dep in jobs[key][2]:
            hear(dep)
        part = lo if d == 0 else hi
        cols = pl.ds(n * (kb // NSUB), kb // NSUB)
        if kind == "y":
            j = key[2]
            r, to = ((0, 3), (3, 2))[st] if d == 0 else ((0, 1), (1, 2))[st]
            take = part if st == 1 else pl.ds(0, rows)
            copies[key] = remote(XB.at[r, j, take, cols], XB.at[to, j, take, cols], Y_SEND, y_recv.at[n, j, st, d],
                                 ydev(1 if d == 0 else -1))
            return
        a, b = (st, st + 1) if d == 0 else ((NX - st) % NX, NX - st - 1)
        take = part if st == HX - 1 else pl.ds(0, rows)
        if kind == "a":
            own_ready("a", n)
            src, dst, sem, recv = XA.at[n, a, take], XA.at[n, b, take], A_SEND, a_recv.at[n, st, d]
        elif kind == "b":
            own_ready("b", 0)
            src, dst, sem, recv = XB.at[0, a, take, cols], XB.at[0, b, take, cols], B_SEND, b_recv.at[n, st, d]
        else:
            src, dst, sem, recv = G.at[a, take], G.at[b, take], G_SEND, g_recv.at[st, d]
        copies[key] = remote(src, dst, sem, recv, xdev(1 if d == 0 else -1))

    started = []

    def gate_up(x, part, sem_l, sem_r):
        for e in range(2):
            both = W.at[e, :, part]
            pltpu.make_async_copy(both, both, sem_l if e == 0 else sem_r).wait()
            for i in range(2):
                y = jnp.dot(x, W[e, i, part, :], preferred_element_type=F32)
                ACC[i, e] = ACC[i, e] + y if started else y
        started.append(1)

    def gate_up_step(key):
        kind, n = key
        for dep in jobs[key][2]:
            hear(dep)
        own_ready(kind[1], n)
        if kind == "ga":
            gate_up(XA[n].reshape(NX * rows, ka), rows_a[n], wla_sem.at[n], wra_sem.at[n])
        else:
            gate_up(XB[n].reshape(NX * rows, kb), rows_b[n], wlb_sem.at[n], wrb_sem.at[n])

    pushes, clock = [], 0.0
    for need, (kind, n) in [(t, key) for t, key in order if jobs[key][0] == 4]:
        for i in range(2):
            pushes.append((min(clock, need - 3.0), "w", (kind, n, i)))
            clock += (ka if kind == "ga" else kb) * hid * 2 / cfg["push_rate"]
    for p in range(NY):
        pushes.append((clock, "d", p))
        clock += ncol * hid * 2 / cfg["push_rate"]
    dr = []

    def push(kind, what):
        if kind == "d":
            dr.append(remote(wd_ref.at[0, :, dcols[what]], WD.at[what, pl.ds(hid, hid)], D_SEND, dr_recv.at[what], partner))
            return
        group, n, i = what
        src, dst, sem = (rows_a[n], rows_a[n], wra_sem.at[n]) if group == "ga" else (from_b[n], rows_b[n], wrb_sem.at[n])
        remote((wg_ref, wu_ref)[i].at[0, src], W.at[1, i, dst], W_SEND, sem, partner)

    events = sorted([(t, 1, n, ("s", key)) for n, (t, key) in enumerate(order)]
                    + [(t, 0, n, (kind, what)) for n, (t, kind, what) in enumerate(pushes)])
    for _, _, _, (kind, what) in events:
        if kind != "s":
            push(kind, what)
        elif jobs[what][0] == 4:
            gate_up_step(what)
        else:
            send(what)
    for d in range(2):
        for st in range(HX):
            hear(("g", 0, st, d))

    g_all = G[...].reshape(NX * rows, 128).astype(F32)
    glane = lax.broadcasted_iota(jnp.int32, (NX * rows, 128), 1)
    grow = lax.broadcasted_iota(jnp.int32, (NX * rows, 128), 0)
    tally = jnp.where((glane == 2 * nexp) & (grow % rows == 0), g_all, 0.0)
    C[0] = jnp.zeros((8, 128), F32) + jnp.sum(tally)
    c_copy = remote(C.at[0], C.at[1], C_SEND, c_recv, partner)
    hs = []
    for e in range(2):
        expert = ep if e == 0 else partner["ep"]
        gate = jnp.sum(jnp.where((glane == expert) | (glane == expert + nexp), g_all, 0.0), axis=1, keepdims=True)
        g, u = ACC[0, e], ACC[1, e]
        hs.append((gate * (g / (1.0 + jnp.exp(-g)) * u)).astype(BF16))
    h = jnp.concatenate(hs, axis=1)

    def down(p):
        dl[p].wait()
        dr[p].wait_recv()
        y = jnp.dot(h, WD[p], preferred_element_type=F32).astype(BF16).reshape(NX, rows, ncol)
        P1[p] = y[:, :half]
        P2[p] = y[:, half:]

    pos = {k: p for p, k in enumerate(kk)}
    NQ = NY // 2
    NJ = NX // 2
    h1, h2 = {}, {}

    def add(dst, src):
        dst[...] = (dst[...].astype(F32) + src[...].astype(F32)).astype(BF16)

    def h1_step(q, s):
        for d in range(2):
            slot = (HX + s) % NX if d == 0 else HX - s
            if s == 0:
                p, n = 2 * q + d, 1
            else:
                p, n = 2 * q, 2
                h1[q, s - 1, d].wait_recv()
                pa, na = (2 * q + d, 1) if s == 1 else (p, n)
                add(P1.at[pl.ds(pa, na), slot], RB1.at[d, s - 1, pl.ds(pa, na)])
            h1[q, s, d] = remote(P1.at[pl.ds(p, n), slot], RB1.at[d, s, pl.ds(p, n)],
                                 H1_SEND, h1_recv.at[q, s, d], xdev(1 if d == 0 else -1))

    def h2_step(j, s):
        for d in range(2):
            p = pos[HY - s] if (d == 0 or s == 0) else pos[s - HY]
            mine = (j < NJ // 2) == (d == 0)
            rng = pl.ds(2 * j, 2)
            if s == 0 and not mine:
                continue
            if s > 0 and (s > 1 or mine):
                h2[j, s - 1, d].wait_recv()
                add(P2.at[p, rng], RB2.at[d, s - 1, rng])
            h2[j, s, d] = remote(P2.at[p, rng], RB2.at[d, s, rng],
                                 H2_SEND, h2_recv.at[j, s, d], ydev(1 if d == 0 else -1))

    down(0)
    for j in range(NJ):
        h2_step(j, 0)
    down(1)
    h1_step(0, 0)
    for q in range(1, NQ):
        down(2 * q)
        down(2 * q + 1)
        h1_step(q, 0)
        if q == 1:
            for j in range(NJ):
                h2_step(j, 1)
    for s in range(1, HX):
        for i in range(max(NQ, NJ)):
            if i < NQ:
                h1_step(i, s)
            if i < NJ and s + 1 < HY:
                h2_step(i, s + 1)

    f1, f2 = [], []
    last = NY - 1

    def h1_final(q):
        h1[q, HX - 1, 0].wait_recv()
        h1[q, HX - 1, 1].wait_recv()
        r = pl.ds(2 * q, 2)
        P1[r, 0] = (P1[r, 0].astype(F32) + RB1[0, HX - 1, r].astype(F32) + RB1[1, HX - 1, r].astype(F32)).astype(BF16)
        for p in (2 * q, 2 * q + 1):
            if kk[p] != 0:
                f1.append(remote(P1.at[p, 0], F1.at[p], F1_SEND, f1_recv.at[p], ydev(kk[p])))

    def h2_final(j):
        h2[j, HY - 1, 0].wait_recv()
        h2[j, HY - 1, 1].wait_recv()
        r = pl.ds(2 * j, 2)
        P2[last, r] = (P2[last, r].astype(F32) + RB2[0, HY - 1, r].astype(F32) + RB2[1, HY - 1, r].astype(F32)).astype(BF16)
        for slot in (2 * j, 2 * j + 1):
            if slot != 0:
                f2.append(remote(P2.at[last, slot], F2.at[slot], F2_SEND, f2_recv.at[slot], xdev(-slot)))

    for i in range(max(NQ, NJ)):
        if i < NJ:
            h2_final(i)
        if i < NQ:
            h1_final(i)

    for c in f1 + f2:
        c.wait_recv()
    a = P1[last, 0].astype(F32)
    for p in range(NY):
        if kk[p] != 0:
            a = a + F1[p].astype(F32)
    out_ref[pl.ds(0, half), :] = a.astype(BF16)
    b = P2[last, 0].astype(F32)
    for slot in range(1, NX):
        b = b + F2[slot].astype(F32)
    out_ref[pl.ds(half, half), :] = b.astype(BF16)
    c_copy.wait_recv()
    first_only = ((lax.broadcasted_iota(jnp.int32, (8, 128), 0) == 0)
                  & (lax.broadcasted_iota(jnp.int32, (8, 128), 1) == 0))
    count_ref[0] = jnp.sum(jnp.where(first_only, C[0] + C[1], 0.0)).astype(jnp.int32)

    def drained(sem, ref):
        pltpu.make_async_copy(ref, ref, send_sem.at[sem]).wait()

    most = pl.ds(0, NX - 1)
    drained(A_SEND, XA.at[:, most])
    drained(B_SEND, XB.at[0, most])
    drained(G_SEND, G.at[most])
    drained(Y_SEND, XB.at[pl.ds(0, 3), most])
    drained(W_SEND, W.at[1])
    drained(D_SEND, WD.at[:, pl.ds(0, hid)])
    drained(C_SEND, C.at[0])
    drained(H1_SEND, P1.at[:, most])
    drained(H2_SEND, P2.at[pl.ds(0, NY - 1)])
    drained(F1_SEND, F1.at[pl.ds(0, NY - 1)])
    drained(F2_SEND, F2.at[most])


def per_device(tokens, w_gate, w_up, w_down, router_logits, expert_ids, draft_lengths, accept_mask):
    nx, ny = lax.axis_size("ep") // 2, lax.axis_size("tp")
    rows, width = tokens.shape
    hid = w_gate.shape[2]
    ncol = width // ny
    half = rows // 2
    hx, hy = nx // 2, ny // 2
    nb, nsub, kb = 4, 2, 1024
    na = 3
    ka = (width - nb * kb) // na
    us_per_col = rows * 2 / 46.6e3
    cfg = dict(nx=nx, ny=ny, na=na, ka=ka, nb=nb, nsub=nsub, kb=kb, rows=rows, ncol=ncol, hid=hid,
               nexp=lax.axis_size("ep"), us_per_col=us_per_col, us_dot=0.6e-3, lat=3.2, push_rate=450e3)
    dma = pltpu.SemaphoreType.DMA
    scratch = [
        pltpu.VMEM((na, nx, rows, ka), BF16),
        pltpu.VMEM((nb, nx, rows, kb), BF16),
        pltpu.VMEM((nx, rows, 128), BF16),
        pltpu.VMEM((2, 2, width, hid), BF16),
        pltpu.VMEM((ny, 2 * hid, ncol), BF16),
        pltpu.VMEM((2, 2, nx * rows, hid), F32),
        pltpu.VMEM((ny, nx, half, ncol), BF16),
        pltpu.VMEM((ny, nx, half, ncol), BF16),
        pltpu.VMEM((2, hx, ny, half, ncol), BF16),
        pltpu.VMEM((2, hy, nx, half, ncol), BF16),
        pltpu.VMEM((ny, half, ncol), BF16),
        pltpu.VMEM((nx, half, ncol), BF16),
        pltpu.VMEM((2, 8, 128), F32),
        dma((na,)), dma((nb,)), dma((na,)), dma((nb,)), dma((na,)), dma((nb,)),
        dma((na, hx, 2)), dma((nsub, hx, 2)), dma((hx, 2)), dma((nsub, nx, 2, 2)), dma((ny // 2, hx, 2)), dma((nx // 2, hy, 2)),
        dma((ny,)), dma((nx,)), dma(()), dma((ny,)), dma((ny,)), dma((11,)),
    ]
    anyspec = pl.BlockSpec(memory_space=pl.ANY)
    vmem = pl.BlockSpec(memory_space=pltpu.VMEM)
    smem = pl.BlockSpec(memory_space=pltpu.SMEM)
    mixed, accepted = pl.pallas_call(
        functools.partial(kernel, cfg),
        out_shape=(jax.ShapeDtypeStruct((rows, ncol), BF16), jax.ShapeDtypeStruct((1,), jnp.int32)),
        in_specs=[anyspec] * 4 + [vmem, vmem, smem, vmem],
        out_specs=(vmem, smem),
        scratch_shapes=scratch,
        name="routed_experts",
        compiler_params=pltpu.CompilerParams(collective_id=0, has_side_effects=True, vmem_limit_bytes=60 * 1024 * 1024),
    )(tokens, w_gate, w_up, w_down, router_logits.T, expert_ids.T, draft_lengths, accept_mask)
    return mixed, accepted


def solution(mesh):
    placed = (
        P(("groups", "ep"), None),
        P("ep", None, "tp"),
        P("ep", None, "tp"),
        P("ep", "tp", None),
        P(("groups", "ep"), None),
        P(("groups", "ep"), None),
        P(("groups", "ep")),
        P(("groups", "ep"), None),
    )
    return jax.shard_map(
        per_device,
        mesh=mesh,
        in_specs=placed,
        out_specs=(P(("groups", "ep"), "tp"), P("groups")),
        check_vma=False,
    )
```

```python
import functools

import jax
import jax.numpy as jnp
from jax import lax
from jax.experimental import pallas as pl
from jax.experimental.pallas import tpu as pltpu
from jax.sharding import PartitionSpec as P

MESH = pl.DeviceIdType.MESH
DRAFT = 8
SCALE = 2.827
BF16, F32 = jnp.bfloat16, jnp.float32


def signed_order(n):
    half = n // 2
    order = [half]
    for d in range(half - 1, 0, -1):
        order += [d, -d]
    return order + [0]


def gather_jobs(nx, na, ka, nb, nsub, kb, us_per_col, us_dot):
    hx = nx // 2
    jobs = {}
    for st in range(hx):
        cut = 0.5 if st == hx - 1 else 1.0
        for d in range(2):
            for q in range(na):
                jobs["a", q, st, d] = (d, ka * us_per_col * cut, [("a", q, st - 1, d)] if st else [], 100 + q)
            for n in range(nsub):
                jobs["b", n, st, d] = (d, kb / nsub * us_per_col * cut, [("b", n, st - 1, d)] if st else [], 0.1 * n)
            jobs["g", 0, st, d] = (d, 128 * us_per_col * cut, [("g", 0, st - 1, d)] if st else [], 1)
    for j in range(1, nx):
        for n in range(nsub):
            dep = [("b", n, st, d) for st, d in ((j - 1, 0), (nx - 1 - j, 1)) if st < hx]
            for d in range(2):
                far = min(j, nx - j)
                jobs["y", n, j, 0, d] = (2 + d, kb / nsub * us_per_col, dep, 10 - far)
                jobs["y", n, j, 1, d] = (2 + d, kb / nsub * us_per_col / 2, [("y", n, j, 0, d)], 9 - far)
    for q in range(na):
        jobs["ga", q] = (4, us_dot * ka, [("a", q, st, d) for st in range(hx) for d in range(2)], 500)
    slots, subs = range(1, nx), range(nsub)
    for r in range(nb):
        if r == 0:
            deps = [("b", n, st, d) for n in subs for st in range(hx) for d in range(2)]
        elif r == 2:
            deps = [("y", n, j, 1, d) for n in subs for j in slots for d in range(2)]
        else:
            deps = [("y", n, j, 0, 0 if r == 3 else 1) for n in subs for j in slots]
        jobs["gb", r] = (4, us_dot * kb, deps, 500)
    return jobs


def scatter_jobs(nx, ny, nq, nj, kk, us_unit, us_down):
    hx, hy = nx // 2, ny // 2
    pos = {k: p for p, k in enumerate(kk)}
    jobs = {("down", p): (4, us_down, [("down", p - 1)] if p else [], p) for p in range(ny)}
    for q in range(nq):
        for st in range(hx):
            for d in range(2):
                deps = [("down", 2 * q + d)] if st == 0 else [("h1", q, st - 1, d), ("down", 2 * q), ("down", 2 * q + 1)]
                jobs["h1", q, st, d] = (d, us_unit * (1 if st == 0 else 2), deps, 600 + st * 10 + q)
        for p in (2 * q, 2 * q + 1):
            if kk[p]:
                jobs["f1", p] = (2 if kk[p] > 0 else 3, us_unit * abs(kk[p]), [("h1", q, hx - 1, 0), ("h1", q, hx - 1, 1)], 700)
    for j in range(nj):
        for st in range(hy):
            for d in range(2):
                mine = (j < nj // 2) == (d == 0)
                if st == 0 and not mine:
                    continue
                deps = [("down", pos[hy - st] if (d == 0 or st == 0) else pos[st - hy])]
                if st > 1 or (st == 1 and mine):
                    deps.append(("h2", j, st - 1, d))
                jobs["h2", j, st, d] = (2 + d, us_unit * 2, deps, 600 + st * 10 + j)
        for slot in (2 * j, 2 * j + 1):
            if slot:
                jobs["f2", slot] = (1 if slot <= hx else 0, us_unit * min(slot, nx - slot),
                                    [("h2", j, hy - 1, 0), ("h2", j, hy - 1, 1), ("down", ny - 1)], 700)
    return jobs


def plan(jobs, lat):
    missing = {k: len(v[2]) for k, v in jobs.items()}
    users = {}
    for k, v in jobs.items():
        for dep in v[2]:
            users.setdefault(dep, []).append(k)
    resources = range(5)
    able = {r: [k for k in jobs if jobs[k][0] == r and not missing[k]] for r in resources}
    when = {k: 0.0 for k in jobs}
    free, order = [0.0 for _ in resources], []
    while len(order) < len(jobs):
        best = None
        for r in resources:
            if able[r]:
                t = max(free[r], min(when[k] for k in able[r]))
                k = min((k for k in able[r] if when[k] <= t + 1e-9), key=lambda k: (jobs[k][3], when[k], k))
                if best is None or t < best[0]:
                    best = (t, k)
        t, k = best
        r = jobs[k][0]
        able[r].remove(k)
        free[r] = t + jobs[k][1]
        order.append((t, k))
        for m in users.get(k, []):
            when[m] = max(when[m], free[r] + (0.0 if r == 4 else lat))
            missing[m] -= 1
            if not missing[m]:
                able[jobs[m][0]].append(m)
    return order


def kernel(cfg, tok_ref, wg_ref, wu_ref, wd_ref, logit_ref, ids_ref, len_ref, mask_ref, out_ref, count_ref,
           XA, XB, G, W, WD, ACC, P1, P2, RB1, RB2, F1, F2, C,
           ta_sem, tb_sem, wla_sem, wlb_sem, wra_sem, wrb_sem, a_recv, b_recv, g_recv, y_recv, h1_recv, h2_recv,
           f1_recv, f2_recv, c_recv, d_sem, dr_recv, send_sem):
    NX, NY, NA, NB, NSUB = cfg["nx"], cfg["ny"], cfg["na"], cfg["nb"], cfg["nsub"]
    HX, HY = NX // 2, NY // 2
    rows = cfg["rows"]
    half = rows // 2
    ka, kb = cfg["ka"], cfg["kb"]
    ncol = cfg["ncol"]
    hid = cfg["hid"]
    nexp = cfg["nexp"]
    n_ep = 2 * NX
    base = NA * ka
    ep = lax.axis_index("ep")
    tp = lax.axis_index("tp")
    core = lax.rem(ep, 2)
    partner = {"ep": ep + 1 - 2 * core}

    def xdev(d):
        there = lax.rem(ep + (2 * d) % n_ep, n_ep)
        return {"ep": there + 1 - 2 * core if d % 2 else there}

    def ydev(d):
        return {"tp": lax.rem(tp + d % NY, NY)}

    def slice_of(r, count, size, start=0):
        return pl.ds(pl.multiple_of(start + lax.rem(tp + r % count, count) * size, 128), size)

    kk = signed_order(NY)
    A_SEND, B_SEND, G_SEND, Y_SEND, H1_SEND, H2_SEND, F1_SEND, F2_SEND, C_SEND, W_SEND, D_SEND = range(11)

    def remote(src, dst, send, recv, dev):
        c = pltpu.make_async_remote_copy(src_ref=src, dst_ref=dst, send_sem=send_sem.at[send], recv_sem=recv,
                                         device_id=dev, device_id_type=MESH)
        c.start()
        return c

    barrier = pltpu.get_barrier_semaphore()
    peers = [partner, xdev(1), xdev(-1), ydev(1), ydev(-1)]
    for dev in peers:
        pl.semaphore_signal(barrier, inc=1, device_id=dev, device_id_type=MESH)

    tok_a, tok_b = [], []
    for r in range(NB):
        c = pltpu.make_async_copy(tok_ref.at[:, slice_of(r, NB, kb, base)], XB.at[r, 0], tb_sem.at[r])
        c.start()
        tok_b.append(c)
    for q in range(NA):
        c = pltpu.make_async_copy(tok_ref.at[:, pl.ds(q * ka, ka)], XA.at[q, 0], ta_sem.at[q])
        c.start()
        tok_a.append(c)
    rows_a = [pl.ds(q * ka, ka) for q in range(NA)]
    rows_b = [pl.ds(base + r * kb, kb) for r in range(NB)]
    from_b = [slice_of(r, NB, kb, base) for r in range(NB)]
    for src, dst, sem in ([(rows_a[q], rows_a[q], wla_sem.at[q]) for q in range(NA)]
                          + [(from_b[r], rows_b[r], wlb_sem.at[r]) for r in range(NB)]):
        for i, w in enumerate((wg_ref, wu_ref)):
            pltpu.make_async_copy(w.at[0, src], W.at[0, i, dst], sem).start()
    dl = []
    dcols = []
    for p in range(NY):
        dcols.append(slice_of(kk[p], NY, ncol))
        c = pltpu.make_async_copy(wd_ref.at[0, :, dcols[p]], WD.at[p, pl.ds(0, hid)], d_sem.at[p])
        c.start()
        dl.append(c)

    def own_gates():
        logits = logit_ref[...]
        sig = 1.0 / (1.0 + jnp.exp(-logits))
        gates = SCALE * sig / jnp.sum(sig, axis=0, keepdims=True)
        lane = lax.broadcasted_iota(jnp.int32, (1, rows), 1)
        length = jnp.zeros((1, rows), jnp.int32)
        for r in range(rows // DRAFT):
            length = jnp.where(lane // DRAFT == r, len_ref[r], length)
        gates = jnp.where(lane % DRAFT < length, gates, 0.0)
        mrow = lax.broadcasted_iota(jnp.int32, mask_ref.shape, 0)
        mcol = lax.broadcasted_iota(jnp.int32, mask_ref.shape, 1)
        mlen = jnp.zeros(mask_ref.shape, jnp.int32)
        for r in range(rows // DRAFT):
            mlen = jnp.where(mrow == r, len_ref[r], mlen)
        passed = jnp.where(mcol < mlen, mask_ref[...], 0).astype(F32)
        run = passed[:, 0:1]
        local_count = run
        for j in range(1, DRAFT):
            run = run * passed[:, j:j + 1]
            local_count = local_count + run
        local_count = jnp.sum(local_count, axis=0, keepdims=True)
        feat = lax.broadcasted_iota(jnp.int32, (128, rows), 0)
        dense = jnp.zeros((128, rows), F32)
        ids = ids_ref[...]
        for k in range(ids.shape[0]):
            e = ids[k:k + 1, :]
            dense = dense + jnp.where((feat == e) | (feat == e + nexp), gates[k:k + 1, :], 0.0)
        high = dense.astype(BF16)
        packed = jnp.where(feat < nexp, high.astype(F32), dense - high.astype(F32))
        packed = packed + jnp.where(feat == 2 * nexp, local_count, 0.0)
        eye = (lax.broadcasted_iota(jnp.int32, (rows, rows), 0) == lax.broadcasted_iota(jnp.int32, (rows, rows), 1))
        turned = lax.dot_general(eye.astype(F32).astype(BF16), packed.astype(BF16), (((1,), (1,)), ((), ())),
                                 preferred_element_type=F32)
        G[0] = turned.astype(BF16)

    pl.semaphore_wait(barrier, len(peers))

    lo, hi = pl.ds(0, half), pl.ds(half, half)
    jobs = gather_jobs(NX, NA, ka, NB, NSUB, kb, cfg["us_per_col"], cfg["us_dot"])
    order = plan(jobs, cfg["lat"])
    copies = {}
    heard = set()

    def hear(key):
        if key not in heard:
            heard.add(key)
            copies[key].wait_recv()

    def own_ready(kind, n):
        if (kind, n) not in heard:
            heard.add((kind, n))
            (tok_a if kind == "a" else tok_b)[n].wait()

    def send(key):
        kind, n, st, d = key[0], key[1], key[-2], key[-1]
        for dep in jobs[key][2]:
            hear(dep)
        part = lo if d == 0 else hi
        cols = pl.ds(n * (kb // NSUB), kb // NSUB)
        if kind == "y":
            j = key[2]
            r, to = ((0, 3), (3, 2))[st] if d == 0 else ((0, 1), (1, 2))[st]
            take = part if st == 1 else pl.ds(0, rows)
            copies[key] = remote(XB.at[r, j, take, cols], XB.at[to, j, take, cols], Y_SEND, y_recv.at[n, j, st, d],
                                 ydev(1 if d == 0 else -1))
            return
        a, b = (st, st + 1) if d == 0 else ((NX - st) % NX, NX - st - 1)
        take = part if st == HX - 1 else pl.ds(0, rows)
        if kind == "a":
            own_ready("a", n)
            src, dst, sem, recv = XA.at[n, a, take], XA.at[n, b, take], A_SEND, a_recv.at[n, st, d]
        elif kind == "b":
            own_ready("b", 0)
            src, dst, sem, recv = XB.at[0, a, take, cols], XB.at[0, b, take, cols], B_SEND, b_recv.at[n, st, d]
        else:
            if "gates" not in heard:
                heard.add("gates")
                own_gates()
            src, dst, sem, recv = G.at[a, take], G.at[b, take], G_SEND, g_recv.at[st, d]
        copies[key] = remote(src, dst, sem, recv, xdev(1 if d == 0 else -1))

    started = []

    def gate_up(x, part, sem_l, sem_r):
        for e in range(2):
            both = W.at[e, :, part]
            pltpu.make_async_copy(both, both, sem_l if e == 0 else sem_r).wait()
            for i in range(2):
                y = jnp.dot(x, W[e, i, part, :], preferred_element_type=F32)
                ACC[i, e] = ACC[i, e] + y if started else y
        started.append(1)

    def gate_up_step(key):
        kind, n = key
        for dep in jobs[key][2]:
            hear(dep)
        own_ready(kind[1], n)
        if kind == "ga":
            gate_up(XA[n].reshape(NX * rows, ka), rows_a[n], wla_sem.at[n], wra_sem.at[n])
        else:
            gate_up(XB[n].reshape(NX * rows, kb), rows_b[n], wlb_sem.at[n], wrb_sem.at[n])

    pushes, clock = [], 0.0
    for need, (kind, n) in [(t, key) for t, key in order if jobs[key][0] == 4]:
        for i in range(2):
            pushes.append((min(clock, need - 3.0), "w", (kind, n, i)))
            clock += (ka if kind == "ga" else kb) * hid * 2 / cfg["push_rate"]
    for p in range(NY):
        pushes.append((clock, "d", p))
        clock += ncol * hid * 2 / cfg["push_rate"]
    dr = []

    def push(kind, what):
        if kind == "d":
            dr.append(remote(wd_ref.at[0, :, dcols[what]], WD.at[what, pl.ds(hid, hid)], D_SEND, dr_recv.at[what], partner))
            return
        group, n, i = what
        src, dst, sem = (rows_a[n], rows_a[n], wra_sem.at[n]) if group == "ga" else (from_b[n], rows_b[n], wrb_sem.at[n])
        remote((wg_ref, wu_ref)[i].at[0, src], W.at[1, i, dst], W_SEND, sem, partner)

    events = sorted([(t, 1, n, ("s", key)) for n, (t, key) in enumerate(order)]
                    + [(t, 0, n, (kind, what)) for n, (t, kind, what) in enumerate(pushes)])
    for _, _, _, (kind, what) in events:
        if kind != "s":
            push(kind, what)
        elif jobs[what][0] == 4:
            gate_up_step(what)
        else:
            send(what)
    for d in range(2):
        for st in range(HX):
            hear(("g", 0, st, d))

    g_all = G[...].reshape(NX * rows, 128).astype(F32)
    glane = lax.broadcasted_iota(jnp.int32, (NX * rows, 128), 1)
    grow = lax.broadcasted_iota(jnp.int32, (NX * rows, 128), 0)
    tally = jnp.where((glane == 2 * nexp) & (grow % rows == 0), g_all, 0.0)
    C[0] = jnp.zeros((8, 128), F32) + jnp.sum(tally)
    c_copy = remote(C.at[0], C.at[1], C_SEND, c_recv, partner)
    hs = []
    for e in range(2):
        expert = ep if e == 0 else partner["ep"]
        gate = jnp.sum(jnp.where((glane == expert) | (glane == expert + nexp), g_all, 0.0), axis=1, keepdims=True)
        g, u = ACC[0, e], ACC[1, e]
        hs.append((gate * (g / (1.0 + jnp.exp(-g)) * u)).astype(BF16))
    h = jnp.concatenate(hs, axis=1)

    def down(p):
        dl[p].wait()
        dr[p].wait_recv()
        y = jnp.dot(h, WD[p], preferred_element_type=F32).astype(BF16).reshape(NX, rows, ncol)
        P1[p] = y[:, :half]
        P2[p] = y[:, half:]

    pos = {k: p for p, k in enumerate(kk)}
    NQ, NJ = NY // 2, NX // 2
    last = NY - 1
    jobs2 = scatter_jobs(NX, NY, NQ, NJ, kk, cfg["us_unit"], cfg["us_down"])
    sent = {}
    done = set()

    def once(key):
        if key in done:
            return False
        done.add(key)
        return True

    def add(dst, *srcs):
        total = dst[...].astype(F32)
        for src in srcs:
            total = total + src[...].astype(F32)
        dst[...] = total.astype(BF16)

    def h1_step(q, s, d):
        slot = (HX + s) % NX if d == 0 else HX - s
        if s == 0:
            p, n = 2 * q + d, 1
        else:
            p, n = 2 * q, 2
            sent["h1", q, s - 1, d].wait_recv()
            pa, na = (2 * q + d, 1) if s == 1 else (p, n)
            add(P1.at[pl.ds(pa, na), slot], RB1.at[d, s - 1, pl.ds(pa, na)])
        sent["h1", q, s, d] = remote(P1.at[pl.ds(p, n), slot], RB1.at[d, s, pl.ds(p, n)], H1_SEND, h1_recv.at[q, s, d],
                                     xdev(1 if d == 0 else -1))

    def h2_step(j, s, d):
        p = pos[HY - s] if (d == 0 or s == 0) else pos[s - HY]
        rng = pl.ds(2 * j, 2)
        if ("h2", j, s - 1, d) in sent:
            sent["h2", j, s - 1, d].wait_recv()
            add(P2.at[p, rng], RB2.at[d, s - 1, rng])
        sent["h2", j, s, d] = remote(P2.at[p, rng], RB2.at[d, s, rng], H2_SEND, h2_recv.at[j, s, d], ydev(1 if d == 0 else -1))

    def h1_final(q):
        if once(("h1", q)):
            sent["h1", q, HX - 1, 0].wait_recv()
            sent["h1", q, HX - 1, 1].wait_recv()
            r = pl.ds(2 * q, 2)
            add(P1.at[r, 0], RB1.at[0, HX - 1, r], RB1.at[1, HX - 1, r])

    def h2_final(j):
        if once(("h2", j)):
            sent["h2", j, HY - 1, 0].wait_recv()
            sent["h2", j, HY - 1, 1].wait_recv()
            r = pl.ds(2 * j, 2)
            add(P2.at[last, r], RB2.at[0, HY - 1, r], RB2.at[1, HY - 1, r])

    f1, f2 = [], []
    for _, key in plan(jobs2, cfg["lat2"]):
        if key[0] == "down":
            down(key[1])
        elif key[0] == "h1":
            h1_step(*key[1:])
        elif key[0] == "h2":
            h2_step(*key[1:])
        elif key[0] == "f1":
            p = key[1]
            h1_final(p // 2)
            f1.append(remote(P1.at[p, 0], F1.at[p], F1_SEND, f1_recv.at[p], ydev(kk[p])))
        else:
            slot = key[1]
            h2_final(slot // 2)
            f2.append(remote(P2.at[last, slot], F2.at[slot], F2_SEND, f2_recv.at[slot], xdev(-slot)))

    for q in range(NQ):
        h1_final(q)
    for j in range(NJ):
        h2_final(j)
    for c in f1 + f2:
        c.wait_recv()
    a = P1[last, 0].astype(F32)
    for p in range(NY):
        if kk[p] != 0:
            a = a + F1[p].astype(F32)
    out_ref[pl.ds(0, half), :] = a.astype(BF16)
    b = P2[last, 0].astype(F32)
    for slot in range(1, NX):
        b = b + F2[slot].astype(F32)
    out_ref[pl.ds(half, half), :] = b.astype(BF16)
    c_copy.wait_recv()
    first_only = ((lax.broadcasted_iota(jnp.int32, (8, 128), 0) == 0)
                  & (lax.broadcasted_iota(jnp.int32, (8, 128), 1) == 0))
    count_ref[0] = jnp.sum(jnp.where(first_only, C[0] + C[1], 0.0)).astype(jnp.int32)

    def drained(sem, ref):
        pltpu.make_async_copy(ref, ref, send_sem.at[sem]).wait()

    most = pl.ds(0, NX - 1)
    drained(A_SEND, XA.at[:, most])
    drained(B_SEND, XB.at[0, most])
    drained(G_SEND, G.at[most])
    drained(Y_SEND, XB.at[pl.ds(0, 3), most])
    drained(W_SEND, W.at[1])
    drained(D_SEND, WD.at[:, pl.ds(0, hid)])
    drained(C_SEND, C.at[0])
    drained(H1_SEND, P1.at[:, most])
    drained(H2_SEND, P2.at[pl.ds(0, NY - 1)])
    drained(F1_SEND, F1.at[pl.ds(0, NY - 1)])
    drained(F2_SEND, F2.at[most])


def per_device(tokens, w_gate, w_up, w_down, router_logits, expert_ids, draft_lengths, accept_mask):
    nx, ny = lax.axis_size("ep") // 2, lax.axis_size("tp")
    rows, width = tokens.shape
    hid = w_gate.shape[2]
    ncol = width // ny
    half = rows // 2
    hx, hy = nx // 2, ny // 2
    nb, nsub, kb = 4, 2, 1024
    na = 3
    ka = (width - nb * kb) // na
    us_per_col = rows * 2 / 46.6e3
    cfg = dict(nx=nx, ny=ny, na=na, ka=ka, nb=nb, nsub=nsub, kb=kb, rows=rows, ncol=ncol, hid=hid,
               nexp=lax.axis_size("ep"), us_per_col=us_per_col, us_dot=0.6e-3, lat=3.2, push_rate=450e3,
               us_unit=half * ncol * 2 / 46.6e3, us_down=0.27, lat2=3.5)
    dma = pltpu.SemaphoreType.DMA
    scratch = [
        pltpu.VMEM((na, nx, rows, ka), BF16),
        pltpu.VMEM((nb, nx, rows, kb), BF16),
        pltpu.VMEM((nx, rows, 128), BF16),
        pltpu.VMEM((2, 2, width, hid), BF16),
        pltpu.VMEM((ny, 2 * hid, ncol), BF16),
        pltpu.VMEM((2, 2, nx * rows, hid), F32),
        pltpu.VMEM((ny, nx, half, ncol), BF16),
        pltpu.VMEM((ny, nx, half, ncol), BF16),
        pltpu.VMEM((2, hx, ny, half, ncol), BF16),
        pltpu.VMEM((2, hy, nx, half, ncol), BF16),
        pltpu.VMEM((ny, half, ncol), BF16),
        pltpu.VMEM((nx, half, ncol), BF16),
        pltpu.VMEM((2, 8, 128), F32),
        dma((na,)), dma((nb,)), dma((na,)), dma((nb,)), dma((na,)), dma((nb,)),
        dma((na, hx, 2)), dma((nsub, hx, 2)), dma((hx, 2)), dma((nsub, nx, 2, 2)), dma((ny // 2, hx, 2)), dma((nx // 2, hy, 2)),
        dma((ny,)), dma((nx,)), dma(()), dma((ny,)), dma((ny,)), dma((11,)),
    ]
    anyspec = pl.BlockSpec(memory_space=pl.ANY)
    vmem = pl.BlockSpec(memory_space=pltpu.VMEM)
    smem = pl.BlockSpec(memory_space=pltpu.SMEM)
    mixed, accepted = pl.pallas_call(
        functools.partial(kernel, cfg),
        out_shape=(jax.ShapeDtypeStruct((rows, ncol), BF16), jax.ShapeDtypeStruct((1,), jnp.int32)),
        in_specs=[anyspec] * 4 + [vmem, vmem, smem, vmem],
        out_specs=(vmem, smem),
        scratch_shapes=scratch,
        name="routed_experts",
        compiler_params=pltpu.CompilerParams(collective_id=0, has_side_effects=True, vmem_limit_bytes=60 * 1024 * 1024),
    )(tokens, w_gate, w_up, w_down, router_logits.T, expert_ids.T, draft_lengths, accept_mask)
    return mixed, accepted


def solution(mesh):
    placed = (
        P(("groups", "ep"), None),
        P("ep", None, "tp"),
        P("ep", None, "tp"),
        P("ep", "tp", None),
        P(("groups", "ep"), None),
        P(("groups", "ep"), None),
        P(("groups", "ep")),
        P(("groups", "ep"), None),
    )
    return jax.shard_map(
        per_device,
        mesh=mesh,
        in_specs=placed,
        out_specs=(P(("groups", "ep"), "tp"), P("groups")),
        check_vma=False,
    )
```

```python
import functools

import jax
import jax.numpy as jnp
from jax import lax
from jax.experimental import pallas as pl
from jax.experimental.pallas import tpu as pltpu
from jax.sharding import PartitionSpec as P

MESH = pl.DeviceIdType.MESH
DRAFT = 8
SCALE = 2.827
BF16, F32 = jnp.bfloat16, jnp.float32


def signed_order(n):
    half = n // 2
    order = [half]
    for d in range(half - 1, 0, -1):
        order += [d, -d]
    return order + [0]


def gather_jobs(nx, na, ka, nb, nsub, kb, us_per_col, us_dot):
    hx = nx // 2
    jobs = {}
    for st in range(hx):
        cut = 0.5 if st == hx - 1 else 1.0
        for d in range(2):
            for q in range(na):
                jobs["a", q, st, d] = (d, ka * us_per_col * cut, [("a", q, st - 1, d)] if st else [], 100 + q)
            for n in range(nsub):
                jobs["b", n, st, d] = (d, kb / nsub * us_per_col * cut, [("b", n, st - 1, d)] if st else [], 0.1 * n)
            jobs["g", 0, st, d] = (d, 128 * us_per_col * cut, [("g", 0, st - 1, d)] if st else [], 1)
    for j in range(1, nx):
        for n in range(nsub):
            dep = [("b", n, st, d) for st, d in ((j - 1, 0), (nx - 1 - j, 1)) if st < hx]
            for d in range(2):
                far = min(j, nx - j)
                jobs["y", n, j, 0, d] = (2 + d, kb / nsub * us_per_col, dep, 10 - far)
                jobs["y", n, j, 1, d] = (2 + d, kb / nsub * us_per_col / 2, [("y", n, j, 0, d)], 9 - far)
    for q in range(na):
        jobs["ga", q] = (4, us_dot * ka, [("a", q, st, d) for st in range(hx) for d in range(2)], 500)
    slots, subs = range(1, nx), range(nsub)
    for r in range(nb):
        if r == 0:
            deps = [("b", n, st, d) for n in subs for st in range(hx) for d in range(2)]
        elif r == 2:
            deps = [("y", n, j, 1, d) for n in subs for j in slots for d in range(2)]
        else:
            deps = [("y", n, j, 0, 0 if r == 3 else 1) for n in subs for j in slots]
        jobs["gb", r] = (4, us_dot * kb, deps, 500)
    return jobs


def scatter_jobs(nx, ny, nq, nj, kk, us_unit, us_down):
    hx, hy = nx // 2, ny // 2
    pos = {k: p for p, k in enumerate(kk)}
    jobs = {("down", p): (4, us_down, [("down", p - 1)] if p else [], p) for p in range(ny)}
    for q in range(nq):
        for st in range(hx):
            for d in range(2):
                deps = [("down", 2 * q + d)] if st == 0 else [("h1", q, st - 1, d), ("down", 2 * q), ("down", 2 * q + 1)]
                jobs["h1", q, st, d] = (d, us_unit * (1 if st == 0 else 2), deps, 600 + st * 10 + q)
        ready = [("h1", q, hx - 1, 0), ("h1", q, hx - 1, 1)]
        for p in (2 * q, 2 * q + 1):
            far = abs(kk[p])
            if far == hy:
                for d in range(2):
                    jobs["e1", d] = (2 + d, us_unit / 2, ready, 500)
            elif far:
                relay = [("e1", 0 if kk[p] > 0 else 1)] if far == hy - 1 else []
                jobs["f1", p] = (2 if kk[p] > 0 else 3, us_unit * far, ready + relay, 700 - far)
    by_distance = sorted(range(nj), key=lambda j: (-max(min(m, nx - m) for m in (2 * j, 2 * j + 1)), j))
    for j in range(nj):
        for st in range(hy):
            for d in range(2):
                mine = (j < nj // 2) == (d == 0)
                if st == 0 and not mine:
                    continue
                deps = [("down", pos[hy - st] if (d == 0 or st == 0) else pos[st - hy])]
                if st > 1 or (st == 1 and mine):
                    deps.append(("h2", j, st - 1, d))
                jobs["h2", j, st, d] = (2 + d, us_unit * 2, deps, 600 + st * 10 + by_distance.index(j))
        ready = [("h2", j, hy - 1, 0), ("h2", j, hy - 1, 1), ("down", ny - 1)]
        for slot in (2 * j, 2 * j + 1):
            far = min(slot, nx - slot)
            if far == hx:
                for d in range(2):
                    jobs["e2", d] = (1 - d, us_unit / 2, ready, 500)
            elif far:
                relay = [("e2", 0 if slot < hx else 1)] if far == hx - 1 else []
                jobs["f2", slot] = (1 if slot < hx else 0, us_unit * far, ready + relay, 700 - far)
    return jobs


def plan(jobs, lat):
    missing = {k: len(v[2]) for k, v in jobs.items()}
    users = {}
    for k, v in jobs.items():
        for dep in v[2]:
            users.setdefault(dep, []).append(k)
    resources = range(5)
    able = {r: [k for k in jobs if jobs[k][0] == r and not missing[k]] for r in resources}
    when = {k: 0.0 for k in jobs}
    free, order = [0.0 for _ in resources], []
    while len(order) < len(jobs):
        best = None
        for r in resources:
            if able[r]:
                t = max(free[r], min(when[k] for k in able[r]))
                k = min((k for k in able[r] if when[k] <= t + 1e-9), key=lambda k: (jobs[k][3], when[k], k))
                if best is None or t < best[0]:
                    best = (t, k)
        t, k = best
        r = jobs[k][0]
        able[r].remove(k)
        free[r] = t + jobs[k][1]
        order.append((t, k))
        for m in users.get(k, []):
            when[m] = max(when[m], free[r] + (0.0 if r == 4 else lat))
            missing[m] -= 1
            if not missing[m]:
                able[jobs[m][0]].append(m)
    return order


def kernel(cfg, tok_ref, wg_ref, wu_ref, wd_ref, logit_ref, ids_ref, len_ref, mask_ref, out_ref, count_ref,
           XA, XB, G, W, WD, ACC, P1, P2, RB1, RB2, F1, F2, E, O, C,
           ta_sem, tb_sem, wla_sem, wlb_sem, wra_sem, wrb_sem, a_recv, b_recv, g_recv, y_recv, h1_recv, h2_recv,
           f1_recv, f2_recv, e_recv, out_sem, c_recv, d_sem, dr_recv, send_sem):
    NX, NY, NA, NB, NSUB = cfg["nx"], cfg["ny"], cfg["na"], cfg["nb"], cfg["nsub"]
    HX, HY = NX // 2, NY // 2
    rows = cfg["rows"]
    half = rows // 2
    ka, kb = cfg["ka"], cfg["kb"]
    ncol = cfg["ncol"]
    hid = cfg["hid"]
    nexp = cfg["nexp"]
    n_ep = 2 * NX
    base = NA * ka
    ep = lax.axis_index("ep")
    tp = lax.axis_index("tp")
    core = lax.rem(ep, 2)
    partner = {"ep": ep + 1 - 2 * core}

    def xdev(d):
        there = lax.rem(ep + (2 * d) % n_ep, n_ep)
        return {"ep": there + 1 - 2 * core if d % 2 else there}

    def ydev(d):
        return {"tp": lax.rem(tp + d % NY, NY)}

    def slice_of(r, count, size, start=0):
        return pl.ds(pl.multiple_of(start + lax.rem(tp + r % count, count) * size, 128), size)

    kk = signed_order(NY)
    A_SEND, B_SEND, G_SEND, Y_SEND, H1_SEND, H2_SEND, F1_SEND, F2_SEND, C_SEND, W_SEND, D_SEND, E_SEND = range(12)

    def remote(src, dst, send, recv, dev):
        c = pltpu.make_async_remote_copy(src_ref=src, dst_ref=dst, send_sem=send_sem.at[send], recv_sem=recv,
                                         device_id=dev, device_id_type=MESH)
        c.start()
        return c

    barrier = pltpu.get_barrier_semaphore()
    peers = [partner, xdev(1), xdev(-1), ydev(1), ydev(-1)]
    for dev in peers:
        pl.semaphore_signal(barrier, inc=1, device_id=dev, device_id_type=MESH)

    tok_a, tok_b = [], []
    for r in range(NB):
        c = pltpu.make_async_copy(tok_ref.at[:, slice_of(r, NB, kb, base)], XB.at[r, 0], tb_sem.at[r])
        c.start()
        tok_b.append(c)
    for q in range(NA):
        c = pltpu.make_async_copy(tok_ref.at[:, pl.ds(q * ka, ka)], XA.at[q, 0], ta_sem.at[q])
        c.start()
        tok_a.append(c)
    rows_a = [pl.ds(q * ka, ka) for q in range(NA)]
    rows_b = [pl.ds(base + r * kb, kb) for r in range(NB)]
    from_b = [slice_of(r, NB, kb, base) for r in range(NB)]
    for src, dst, sem in ([(rows_a[q], rows_a[q], wla_sem.at[q]) for q in range(NA)]
                          + [(from_b[r], rows_b[r], wlb_sem.at[r]) for r in range(NB)]):
        for i, w in enumerate((wg_ref, wu_ref)):
            pltpu.make_async_copy(w.at[0, src], W.at[0, i, dst], sem).start()
    dl = []
    dcols = []
    for p in range(NY):
        dcols.append(slice_of(kk[p], NY, ncol))
        c = pltpu.make_async_copy(wd_ref.at[0, :, dcols[p]], WD.at[p, pl.ds(0, hid)], d_sem.at[p])
        c.start()
        dl.append(c)

    def own_gates():
        logits = logit_ref[...]
        sig = 1.0 / (1.0 + jnp.exp(-logits))
        gates = SCALE * sig / jnp.sum(sig, axis=0, keepdims=True)
        lane = lax.broadcasted_iota(jnp.int32, (1, rows), 1)
        length = jnp.zeros((1, rows), jnp.int32)
        for r in range(rows // DRAFT):
            length = jnp.where(lane // DRAFT == r, len_ref[r], length)
        gates = jnp.where(lane % DRAFT < length, gates, 0.0)
        mrow = lax.broadcasted_iota(jnp.int32, mask_ref.shape, 0)
        mcol = lax.broadcasted_iota(jnp.int32, mask_ref.shape, 1)
        mlen = jnp.zeros(mask_ref.shape, jnp.int32)
        for r in range(rows // DRAFT):
            mlen = jnp.where(mrow == r, len_ref[r], mlen)
        passed = jnp.where(mcol < mlen, mask_ref[...], 0).astype(F32)
        run = passed[:, 0:1]
        local_count = run
        for j in range(1, DRAFT):
            run = run * passed[:, j:j + 1]
            local_count = local_count + run
        local_count = jnp.sum(local_count, axis=0, keepdims=True)
        feat = lax.broadcasted_iota(jnp.int32, (128, rows), 0)
        dense = jnp.zeros((128, rows), F32)
        ids = ids_ref[...]
        for k in range(ids.shape[0]):
            e = ids[k:k + 1, :]
            dense = dense + jnp.where((feat == e) | (feat == e + nexp), gates[k:k + 1, :], 0.0)
        high = dense.astype(BF16)
        packed = jnp.where(feat < nexp, high.astype(F32), dense - high.astype(F32))
        packed = packed + jnp.where(feat == 2 * nexp, local_count, 0.0)
        eye = (lax.broadcasted_iota(jnp.int32, (rows, rows), 0) == lax.broadcasted_iota(jnp.int32, (rows, rows), 1))
        turned = lax.dot_general(eye.astype(F32).astype(BF16), packed.astype(BF16), (((1,), (1,)), ((), ())),
                                 preferred_element_type=F32)
        G[0] = turned.astype(BF16)

    pl.semaphore_wait(barrier, len(peers))

    lo, hi = pl.ds(0, half), pl.ds(half, half)
    jobs = gather_jobs(NX, NA, ka, NB, NSUB, kb, cfg["us_per_col"], cfg["us_dot"])
    order = plan(jobs, cfg["lat"])
    copies = {}
    heard = set()

    def hear(key):
        if key not in heard:
            heard.add(key)
            copies[key].wait_recv()

    def own_ready(kind, n):
        if (kind, n) not in heard:
            heard.add((kind, n))
            (tok_a if kind == "a" else tok_b)[n].wait()

    def send(key):
        kind, n, st, d = key[0], key[1], key[-2], key[-1]
        for dep in jobs[key][2]:
            hear(dep)
        part = lo if d == 0 else hi
        cols = pl.ds(n * (kb // NSUB), kb // NSUB)
        if kind == "y":
            j = key[2]
            r, to = ((0, 3), (3, 2))[st] if d == 0 else ((0, 1), (1, 2))[st]
            take = part if st == 1 else pl.ds(0, rows)
            copies[key] = remote(XB.at[r, j, take, cols], XB.at[to, j, take, cols], Y_SEND, y_recv.at[n, j, st, d],
                                 ydev(1 if d == 0 else -1))
            return
        a, b = (st, st + 1) if d == 0 else ((NX - st) % NX, NX - st - 1)
        take = part if st == HX - 1 else pl.ds(0, rows)
        if kind == "a":
            own_ready("a", n)
            src, dst, sem, recv = XA.at[n, a, take], XA.at[n, b, take], A_SEND, a_recv.at[n, st, d]
        elif kind == "b":
            own_ready("b", 0)
            src, dst, sem, recv = XB.at[0, a, take, cols], XB.at[0, b, take, cols], B_SEND, b_recv.at[n, st, d]
        else:
            if "gates" not in heard:
                heard.add("gates")
                own_gates()
            src, dst, sem, recv = G.at[a, take], G.at[b, take], G_SEND, g_recv.at[st, d]
        copies[key] = remote(src, dst, sem, recv, xdev(1 if d == 0 else -1))

    started = []

    def gate_up(x, part, sem_l, sem_r):
        for e in range(2):
            both = W.at[e, :, part]
            pltpu.make_async_copy(both, both, sem_l if e == 0 else sem_r).wait()
            for i in range(2):
                y = jnp.dot(x, W[e, i, part, :], preferred_element_type=F32)
                ACC[i, e] = ACC[i, e] + y if started else y
        started.append(1)

    def gate_up_step(key):
        kind, n = key
        for dep in jobs[key][2]:
            hear(dep)
        own_ready(kind[1], n)
        if kind == "ga":
            gate_up(XA[n].reshape(NX * rows, ka), rows_a[n], wla_sem.at[n], wra_sem.at[n])
        else:
            gate_up(XB[n].reshape(NX * rows, kb), rows_b[n], wlb_sem.at[n], wrb_sem.at[n])

    pushes, clock = [], 0.0
    for need, (kind, n) in [(t, key) for t, key in order if jobs[key][0] == 4]:
        for i in range(2):
            pushes.append((min(clock, need - 3.0), "w", (kind, n, i)))
            clock += (ka if kind == "ga" else kb) * hid * 2 / cfg["push_rate"]
    for p in range(NY):
        pushes.append((clock, "d", p))
        clock += ncol * hid * 2 / cfg["push_rate"]
    dr = []

    def push(kind, what):
        if kind == "d":
            dr.append(remote(wd_ref.at[0, :, dcols[what]], WD.at[what, pl.ds(hid, hid)], D_SEND, dr_recv.at[what], partner))
            return
        group, n, i = what
        src, dst, sem = (rows_a[n], rows_a[n], wra_sem.at[n]) if group == "ga" else (from_b[n], rows_b[n], wrb_sem.at[n])
        remote((wg_ref, wu_ref)[i].at[0, src], W.at[1, i, dst], W_SEND, sem, partner)

    events = sorted([(t, 1, n, ("s", key)) for n, (t, key) in enumerate(order)]
                    + [(t, 0, n, (kind, what)) for n, (t, kind, what) in enumerate(pushes)])
    for _, _, _, (kind, what) in events:
        if kind != "s":
            push(kind, what)
        elif jobs[what][0] == 4:
            gate_up_step(what)
        else:
            send(what)
    for d in range(2):
        for st in range(HX):
            hear(("g", 0, st, d))

    g_all = G[...].reshape(NX * rows, 128).astype(F32)
    glane = lax.broadcasted_iota(jnp.int32, (NX * rows, 128), 1)
    grow = lax.broadcasted_iota(jnp.int32, (NX * rows, 128), 0)
    tally = jnp.where((glane == 2 * nexp) & (grow % rows == 0), g_all, 0.0)
    C[0] = jnp.zeros((8, 128), F32) + jnp.sum(tally)
    c_copy = remote(C.at[0], C.at[1], C_SEND, c_recv, partner)
    hs = []
    for e in range(2):
        expert = ep if e == 0 else partner["ep"]
        gate = jnp.sum(jnp.where((glane == expert) | (glane == expert + nexp), g_all, 0.0), axis=1, keepdims=True)
        g, u = ACC[0, e], ACC[1, e]
        hs.append((gate * (g / (1.0 + jnp.exp(-g)) * u)).astype(BF16))
    h = jnp.concatenate(hs, axis=1)

    def down(p):
        dl[p].wait()
        dr[p].wait_recv()
        y = jnp.dot(h, WD[p], preferred_element_type=F32).astype(BF16).reshape(NX, rows, ncol)
        P1[p] = y[:, :half]
        P2[p] = y[:, half:]

    pos = {k: p for p, k in enumerate(kk)}
    NQ, NJ = NY // 2, NX // 2
    last = NY - 1
    jobs2 = scatter_jobs(NX, NY, NQ, NJ, kk, cfg["us_unit"], cfg["us_down"])
    sent = {}
    done = set()

    def once(key):
        if key in done:
            return False
        done.add(key)
        return True

    def add(dst, *srcs):
        total = dst[...].astype(F32)
        for src in srcs:
            total = total + src[...].astype(F32)
        dst[...] = total.astype(BF16)

    def h1_step(q, s, d):
        slot = (HX + s) % NX if d == 0 else HX - s
        if s == 0:
            p, n = 2 * q + d, 1
        else:
            p, n = 2 * q, 2
            sent["h1", q, s - 1, d].wait_recv()
            pa, na = (2 * q + d, 1) if s == 1 else (p, n)
            add(P1.at[pl.ds(pa, na), slot], RB1.at[d, s - 1, pl.ds(pa, na)])
        sent["h1", q, s, d] = remote(P1.at[pl.ds(p, n), slot], RB1.at[d, s, pl.ds(p, n)], H1_SEND, h1_recv.at[q, s, d],
                                     xdev(1 if d == 0 else -1))

    def h2_step(j, s, d):
        p = pos[HY - s] if (d == 0 or s == 0) else pos[s - HY]
        rng = pl.ds(2 * j, 2)
        if ("h2", j, s - 1, d) in sent:
            sent["h2", j, s - 1, d].wait_recv()
            add(P2.at[p, rng], RB2.at[d, s - 1, rng])
        sent["h2", j, s, d] = remote(P2.at[p, rng], RB2.at[d, s, rng], H2_SEND, h2_recv.at[j, s, d], ydev(1 if d == 0 else -1))

    def h1_final(q):
        if once(("h1", q)):
            sent["h1", q, HX - 1, 0].wait_recv()
            sent["h1", q, HX - 1, 1].wait_recv()
            r = pl.ds(2 * q, 2)
            add(P1.at[r, 0], RB1.at[0, HX - 1, r], RB1.at[1, HX - 1, r])

    def h2_final(j):
        if once(("h2", j)):
            sent["h2", j, HY - 1, 0].wait_recv()
            sent["h2", j, HY - 1, 1].wait_recv()
            r = pl.ds(2 * j, 2)
            add(P2.at[last, r], RB2.at[0, HY - 1, r], RB2.at[1, HY - 1, r])

    f1, f2 = [], []
    cut = -(-(ncol // 128) // 2) * 128
    parts = (pl.ds(0, cut), pl.ds(cut, ncol - cut))
    for _, key in plan(jobs2, cfg["lat2"]):
        if key[0] == "down":
            down(key[1])
        elif key[0] == "h1":
            h1_step(*key[1:])
        elif key[0] == "h2":
            h2_step(*key[1:])
        elif key[0] == "e1":
            d = key[1]
            h1_final(pos[HY] // 2)
            sent[key] = remote(P1.at[pos[HY], 0, :, parts[d]], E.at[0, :, parts[d]], E_SEND, e_recv.at[0, d],
                               ydev(1 if d == 0 else -1))
        elif key[0] == "e2":
            d = key[1]
            h2_final(HX // 2)
            sent[key] = remote(P2.at[last, HX, :, parts[d]], E.at[1, :, parts[d]], E_SEND, e_recv.at[1, d],
                               xdev(-1 if d == 0 else 1))
        elif key[0] == "f1":
            p = key[1]
            h1_final(p // 2)
            if abs(kk[p]) == HY - 1:
                d = 0 if kk[p] > 0 else 1
                sent["e1", d].wait_recv()
                add(P1.at[p, 0, :, parts[d]], E.at[0, :, parts[d]])
            f1.append((p, remote(P1.at[p, 0], F1.at[p], F1_SEND, f1_recv.at[p], ydev(kk[p]))))
        else:
            slot = key[1]
            h2_final(slot // 2)
            if min(slot, NX - slot) == HX - 1:
                d = 0 if slot < HX else 1
                sent["e2", d].wait_recv()
                add(P2.at[last, slot, :, parts[d]], E.at[1, :, parts[d]])
            f2.append((slot, remote(P2.at[last, slot], F2.at[slot], F2_SEND, f2_recv.at[slot], xdev(-slot))))

    for q in range(NQ):
        h1_final(q)
    for j in range(NJ):
        h2_final(j)
    out_copies = []
    for n, (own, arrived, ref) in enumerate(((P1.at[last, 0], f1, F1), (P2.at[last, 0], f2, F2))):
        total = own[...].astype(F32)
        for m, c in arrived:
            c.wait_recv()
            total = total + ref[m].astype(F32)
        O[n] = total.astype(BF16)
        c = pltpu.make_async_copy(O.at[n], out_ref.at[pl.ds(n * half, half)], out_sem.at[n])
        c.start()
        out_copies.append(c)
    c_copy.wait_recv()
    first_only = ((lax.broadcasted_iota(jnp.int32, (8, 128), 0) == 0)
                  & (lax.broadcasted_iota(jnp.int32, (8, 128), 1) == 0))
    count_ref[0] = jnp.sum(jnp.where(first_only, C[0] + C[1], 0.0)).astype(jnp.int32)

    def drained(sem, ref):
        pltpu.make_async_copy(ref, ref, send_sem.at[sem]).wait()

    most = pl.ds(0, NX - 1)
    drained(A_SEND, XA.at[:, most])
    drained(B_SEND, XB.at[0, most])
    drained(G_SEND, G.at[most])
    drained(Y_SEND, XB.at[pl.ds(0, 3), most])
    drained(W_SEND, W.at[1])
    drained(D_SEND, WD.at[:, pl.ds(0, hid)])
    drained(C_SEND, C.at[0])
    drained(H1_SEND, P1.at[:, most])
    drained(H2_SEND, P2.at[pl.ds(0, NY - 1)])
    drained(E_SEND, E)
    drained(F1_SEND, F1.at[pl.ds(0, NY - 2)])
    drained(F2_SEND, F2.at[pl.ds(0, NX - 2)])
    for c in out_copies:
        c.wait()


def per_device(tokens, w_gate, w_up, w_down, router_logits, expert_ids, draft_lengths, accept_mask):
    nx, ny = lax.axis_size("ep") // 2, lax.axis_size("tp")
    rows, width = tokens.shape
    hid = w_gate.shape[2]
    ncol = width // ny
    half = rows // 2
    hx, hy = nx // 2, ny // 2
    nb, nsub, kb = 4, 2, 1024
    na = 3
    ka = (width - nb * kb) // na
    us_per_col = rows * 2 / 46.6e3
    cfg = dict(nx=nx, ny=ny, na=na, ka=ka, nb=nb, nsub=nsub, kb=kb, rows=rows, ncol=ncol, hid=hid,
               nexp=lax.axis_size("ep"), us_per_col=us_per_col, us_dot=0.6e-3, lat=3.2, push_rate=450e3,
               us_unit=half * ncol * 2 / 46.6e3, us_down=0.27, lat2=2.4)
    dma = pltpu.SemaphoreType.DMA
    scratch = [
        pltpu.VMEM((na, nx, rows, ka), BF16),
        pltpu.VMEM((nb, nx, rows, kb), BF16),
        pltpu.VMEM((nx, rows, 128), BF16),
        pltpu.VMEM((2, 2, width, hid), BF16),
        pltpu.VMEM((ny, 2 * hid, ncol), BF16),
        pltpu.VMEM((2, 2, nx * rows, hid), F32),
        pltpu.VMEM((ny, nx, half, ncol), BF16),
        pltpu.VMEM((ny, nx, half, ncol), BF16),
        pltpu.VMEM((2, hx, ny, half, ncol), BF16),
        pltpu.VMEM((2, hy, nx, half, ncol), BF16),
        pltpu.VMEM((ny, half, ncol), BF16),
        pltpu.VMEM((nx, half, ncol), BF16),
        pltpu.VMEM((2, half, ncol), BF16),
        pltpu.VMEM((2, half, ncol), BF16),
        pltpu.VMEM((2, 8, 128), F32),
        dma((na,)), dma((nb,)), dma((na,)), dma((nb,)), dma((na,)), dma((nb,)),
        dma((na, hx, 2)), dma((nsub, hx, 2)), dma((hx, 2)), dma((nsub, nx, 2, 2)), dma((ny // 2, hx, 2)), dma((nx // 2, hy, 2)),
        dma((ny,)), dma((nx,)), dma((2, 2)), dma((2,)), dma(()), dma((ny,)), dma((ny,)), dma((12,)),
    ]
    anyspec = pl.BlockSpec(memory_space=pl.ANY)
    vmem = pl.BlockSpec(memory_space=pltpu.VMEM)
    smem = pl.BlockSpec(memory_space=pltpu.SMEM)
    mixed, accepted = pl.pallas_call(
        functools.partial(kernel, cfg),
        out_shape=(jax.ShapeDtypeStruct((rows, ncol), BF16), jax.ShapeDtypeStruct((1,), jnp.int32)),
        in_specs=[anyspec] * 4 + [vmem, vmem, smem, vmem],
        out_specs=(anyspec, smem),
        scratch_shapes=scratch,
        name="routed_experts",
        compiler_params=pltpu.CompilerParams(collective_id=0, has_side_effects=True, vmem_limit_bytes=60 * 1024 * 1024),
    )(tokens, w_gate, w_up, w_down, router_logits.T, expert_ids.T, draft_lengths, accept_mask)
    return mixed, accepted


def solution(mesh):
    placed = (
        P(("groups", "ep"), None),
        P("ep", None, "tp"),
        P("ep", None, "tp"),
        P("ep", "tp", None),
        P(("groups", "ep"), None),
        P(("groups", "ep"), None),
        P(("groups", "ep")),
        P(("groups", "ep"), None),
    )
    return jax.shard_map(
        per_device,
        mesh=mesh,
        in_specs=placed,
        out_specs=(P(("groups", "ep"), "tp"), P("groups")),
        check_vma=False,
    )
```

```python
import functools

import jax
import jax.numpy as jnp
from jax import lax
from jax.experimental import pallas as pl
from jax.experimental.pallas import tpu as pltpu
from jax.sharding import PartitionSpec as P

MESH = pl.DeviceIdType.MESH
DRAFT = 8
SCALE = 2.827
BF16, F32 = jnp.bfloat16, jnp.float32


def signed_order(n):
    half = n // 2
    order = [half]
    for d in range(half - 1, 0, -1):
        order += [d, -d]
    return order + [0]


def gather_jobs(nx, na, ka, nb, nsub, kb, us_per_col, us_dot):
    hx = nx // 2
    jobs = {}
    for st in range(hx):
        cut = 0.5 if st == hx - 1 else 1.0
        for d in range(2):
            for q in range(na):
                jobs["a", q, st, d] = (d, ka * us_per_col * cut, [("a", q, st - 1, d)] if st else [], 100 + q)
            for n in range(nsub):
                jobs["b", n, st, d] = (d, kb / nsub * us_per_col * cut, [("b", n, st - 1, d)] if st else [], 0.1 * n)
            jobs["g", 0, st, d] = (d, 128 * us_per_col * cut, [("g", 0, st - 1, d)] if st else [], 1)
    for j in range(1, nx):
        for n in range(nsub):
            dep = [("b", n, st, d) for st, d in ((j - 1, 0), (nx - 1 - j, 1)) if st < hx]
            for d in range(2):
                far = min(j, nx - j)
                jobs["y", n, j, 0, d] = (2 + d, kb / nsub * us_per_col, dep, 10 - far)
                jobs["y", n, j, 1, d] = (2 + d, kb / nsub * us_per_col / 2, [("y", n, j, 0, d)], 9 - far)
    for q in range(na):
        jobs["ga", q] = (4, us_dot * ka, [("a", q, st, d) for st in range(hx) for d in range(2)], 500)
    slots, subs = range(1, nx), range(nsub)
    for r in range(nb):
        if r == 0:
            deps = [("b", n, st, d) for n in subs for st in range(hx) for d in range(2)]
        elif r == 2:
            deps = [("y", n, j, 1, d) for n in subs for j in slots for d in range(2)]
        else:
            deps = [("y", n, j, 0, 0 if r == 3 else 1) for n in subs for j in slots]
        jobs["gb", r] = (4, us_dot * kb, deps, 500)
    return jobs


def scatter_jobs(nx, ny, nq, nj, kk, us_unit, us_down):
    hx, hy = nx // 2, ny // 2
    pos = {k: p for p, k in enumerate(kk)}
    jobs = {("down", p): (4, us_down, [("down", p - 1)] if p else [], p) for p in range(ny)}
    for q in range(nq):
        for st in range(hx):
            for d in range(2):
                deps = [("down", 2 * q + d)] if st == 0 else [("h1", q, st - 1, d), ("down", 2 * q), ("down", 2 * q + 1)]
                jobs["h1", q, st, d] = (d, us_unit * (1 if st == 0 else 2), deps, 600 + st * 10 + q)
        ready = [("h1", q, hx - 1, 0), ("h1", q, hx - 1, 1)]
        for p in (2 * q, 2 * q + 1):
            far = abs(kk[p])
            if far == hy:
                for d in range(2):
                    jobs["e1", d] = (2 + d, us_unit / 2, ready, 500)
            elif far:
                relay = [("e1", 0 if kk[p] > 0 else 1)] if far == hy - 1 else []
                jobs["f1", p] = (2 if kk[p] > 0 else 3, us_unit * far, ready + relay, 700 - far)
    by_distance = sorted(range(nj), key=lambda j: (-max(min(m, nx - m) for m in (2 * j, 2 * j + 1)), j))
    for j in range(nj):
        for st in range(hy):
            for d in range(2):
                mine = (j < nj // 2) == (d == 0)
                if st == 0 and not mine:
                    continue
                deps = [("down", pos[hy - st] if (d == 0 or st == 0) else pos[st - hy])]
                if st > 1 or (st == 1 and mine):
                    deps.append(("h2", j, st - 1, d))
                jobs["h2", j, st, d] = (2 + d, us_unit * 2, deps, 600 + st * 10 + by_distance.index(j))
        ready = [("h2", j, hy - 1, 0), ("h2", j, hy - 1, 1), ("down", ny - 1)]
        for slot in (2 * j, 2 * j + 1):
            far = min(slot, nx - slot)
            if far == hx:
                for d in range(2):
                    jobs["e2", d] = (1 - d, us_unit / 2, ready, 500)
            elif far:
                relay = [("e2", 0 if slot < hx else 1)] if far == hx - 1 else []
                jobs["f2", slot] = (1 if slot < hx else 0, us_unit * far, ready + relay, 700 - far)
    return jobs


def plan(jobs, lat):
    missing = {k: len(v[2]) for k, v in jobs.items()}
    users = {}
    for k, v in jobs.items():
        for dep in v[2]:
            users.setdefault(dep, []).append(k)
    resources = range(5)
    able = {r: [k for k in jobs if jobs[k][0] == r and not missing[k]] for r in resources}
    when = {k: 0.0 for k in jobs}
    free, order = [0.0 for _ in resources], []
    while len(order) < len(jobs):
        best = None
        for r in resources:
            if able[r]:
                t = max(free[r], min(when[k] for k in able[r]))
                k = min((k for k in able[r] if when[k] <= t + 1e-9), key=lambda k: (jobs[k][3], when[k], k))
                if best is None or t < best[0]:
                    best = (t, k)
        t, k = best
        r = jobs[k][0]
        able[r].remove(k)
        free[r] = t + jobs[k][1]
        order.append((t, k))
        for m in users.get(k, []):
            when[m] = max(when[m], free[r] + (0.0 if r == 4 else lat))
            missing[m] -= 1
            if not missing[m]:
                able[jobs[m][0]].append(m)
    return order


def kernel(cfg, tok_ref, wg_ref, wu_ref, wd_ref, logit_ref, ids_ref, len_ref, mask_ref, out_ref, count_ref,
           XA, XB, G, W, WD, ACC, P1, P2, RB1, RB2, F1, F2, E, C,
           ta_sem, tb_sem, wla_sem, wlb_sem, wra_sem, wrb_sem, a_recv, b_recv, g_recv, y_recv, h1_recv, h2_recv,
           f1_recv, f2_recv, e_recv, c_recv, d_sem, dr_recv, send_sem):
    NX, NY, NA, NB, NSUB = cfg["nx"], cfg["ny"], cfg["na"], cfg["nb"], cfg["nsub"]
    HX, HY = NX // 2, NY // 2
    rows = cfg["rows"]
    half = rows // 2
    ka, kb = cfg["ka"], cfg["kb"]
    ncol = cfg["ncol"]
    hid = cfg["hid"]
    nexp = cfg["nexp"]
    n_ep = 2 * NX
    base = NA * ka
    ep = lax.axis_index("ep")
    tp = lax.axis_index("tp")
    core = lax.rem(ep, 2)
    partner = {"ep": ep + 1 - 2 * core}

    def xdev(d):
        there = lax.rem(ep + (2 * d) % n_ep, n_ep)
        return {"ep": there + 1 - 2 * core if d % 2 else there}

    def ydev(d):
        return {"tp": lax.rem(tp + d % NY, NY)}

    def slice_of(r, count, size, start=0):
        return pl.ds(pl.multiple_of(start + lax.rem(tp + r % count, count) * size, 128), size)

    kk = signed_order(NY)
    A_SEND, B_SEND, G_SEND, Y_SEND, H1_SEND, H2_SEND, F1_SEND, F2_SEND, C_SEND, W_SEND, D_SEND, E_SEND = range(12)

    def remote(src, dst, send, recv, dev):
        c = pltpu.make_async_remote_copy(src_ref=src, dst_ref=dst, send_sem=send_sem.at[send], recv_sem=recv,
                                         device_id=dev, device_id_type=MESH)
        c.start()
        return c

    barrier = pltpu.get_barrier_semaphore()
    peers = [partner, xdev(1), xdev(-1), ydev(1), ydev(-1)]
    for dev in peers:
        pl.semaphore_signal(barrier, inc=1, device_id=dev, device_id_type=MESH)

    tok_a, tok_b = [], []
    for r in range(NB):
        c = pltpu.make_async_copy(tok_ref.at[:, slice_of(r, NB, kb, base)], XB.at[r, 0], tb_sem.at[r])
        c.start()
        tok_b.append(c)
    for q in range(NA):
        c = pltpu.make_async_copy(tok_ref.at[:, pl.ds(q * ka, ka)], XA.at[q, 0], ta_sem.at[q])
        c.start()
        tok_a.append(c)
    rows_a = [pl.ds(q * ka, ka) for q in range(NA)]
    rows_b = [pl.ds(base + r * kb, kb) for r in range(NB)]
    from_b = [slice_of(r, NB, kb, base) for r in range(NB)]
    for src, dst, sem in ([(rows_a[q], rows_a[q], wla_sem.at[q]) for q in range(NA)]
                          + [(from_b[r], rows_b[r], wlb_sem.at[r]) for r in range(NB)]):
        for i, w in enumerate((wg_ref, wu_ref)):
            pltpu.make_async_copy(w.at[0, src], W.at[0, i, dst], sem).start()
    dl = []
    dcols = []
    for p in range(NY):
        dcols.append(slice_of(kk[p], NY, ncol))
        c = pltpu.make_async_copy(wd_ref.at[0, :, dcols[p]], WD.at[p, pl.ds(0, hid)], d_sem.at[p])
        c.start()
        dl.append(c)

    def own_gates():
        logits = logit_ref[...]
        sig = 1.0 / (1.0 + jnp.exp(-logits))
        gates = SCALE * sig / jnp.sum(sig, axis=0, keepdims=True)
        lane = lax.broadcasted_iota(jnp.int32, (1, rows), 1)
        length = jnp.zeros((1, rows), jnp.int32)
        for r in range(rows // DRAFT):
            length = jnp.where(lane // DRAFT == r, len_ref[r], length)
        gates = jnp.where(lane % DRAFT < length, gates, 0.0)
        mrow = lax.broadcasted_iota(jnp.int32, mask_ref.shape, 0)
        mcol = lax.broadcasted_iota(jnp.int32, mask_ref.shape, 1)
        mlen = jnp.zeros(mask_ref.shape, jnp.int32)
        for r in range(rows // DRAFT):
            mlen = jnp.where(mrow == r, len_ref[r], mlen)
        passed = jnp.where(mcol < mlen, mask_ref[...], 0).astype(F32)
        run = passed[:, 0:1]
        local_count = run
        for j in range(1, DRAFT):
            run = run * passed[:, j:j + 1]
            local_count = local_count + run
        local_count = jnp.sum(local_count, axis=0, keepdims=True)
        feat = lax.broadcasted_iota(jnp.int32, (128, rows), 0)
        dense = jnp.zeros((128, rows), F32)
        ids = ids_ref[...]
        for k in range(ids.shape[0]):
            e = ids[k:k + 1, :]
            dense = dense + jnp.where((feat == e) | (feat == e + nexp), gates[k:k + 1, :], 0.0)
        high = dense.astype(BF16)
        packed = jnp.where(feat < nexp, high.astype(F32), dense - high.astype(F32))
        packed = packed + jnp.where(feat == 2 * nexp, local_count, 0.0)
        eye = (lax.broadcasted_iota(jnp.int32, (rows, rows), 0) == lax.broadcasted_iota(jnp.int32, (rows, rows), 1))
        turned = lax.dot_general(eye.astype(F32).astype(BF16), packed.astype(BF16), (((1,), (1,)), ((), ())),
                                 preferred_element_type=F32)
        G[0] = turned.astype(BF16)

    pl.semaphore_wait(barrier, len(peers))

    lo, hi = pl.ds(0, half), pl.ds(half, half)
    jobs = gather_jobs(NX, NA, ka, NB, NSUB, kb, cfg["us_per_col"], cfg["us_dot"])
    order = plan(jobs, cfg["lat"])
    copies = {}
    heard = set()

    def hear(key):
        if key not in heard:
            heard.add(key)
            copies[key].wait_recv()

    def own_ready(kind, n):
        if (kind, n) not in heard:
            heard.add((kind, n))
            (tok_a if kind == "a" else tok_b)[n].wait()

    def send(key):
        kind, n, st, d = key[0], key[1], key[-2], key[-1]
        for dep in jobs[key][2]:
            hear(dep)
        part = lo if d == 0 else hi
        cols = pl.ds(n * (kb // NSUB), kb // NSUB)
        if kind == "y":
            j = key[2]
            r, to = ((0, 3), (3, 2))[st] if d == 0 else ((0, 1), (1, 2))[st]
            take = part if st == 1 else pl.ds(0, rows)
            copies[key] = remote(XB.at[r, j, take, cols], XB.at[to, j, take, cols], Y_SEND, y_recv.at[n, j, st, d],
                                 ydev(1 if d == 0 else -1))
            return
        a, b = (st, st + 1) if d == 0 else ((NX - st) % NX, NX - st - 1)
        take = part if st == HX - 1 else pl.ds(0, rows)
        if kind == "a":
            own_ready("a", n)
            src, dst, sem, recv = XA.at[n, a, take], XA.at[n, b, take], A_SEND, a_recv.at[n, st, d]
        elif kind == "b":
            own_ready("b", 0)
            src, dst, sem, recv = XB.at[0, a, take, cols], XB.at[0, b, take, cols], B_SEND, b_recv.at[n, st, d]
        else:
            if "gates" not in heard:
                heard.add("gates")
                own_gates()
            src, dst, sem, recv = G.at[a, take], G.at[b, take], G_SEND, g_recv.at[st, d]
        copies[key] = remote(src, dst, sem, recv, xdev(1 if d == 0 else -1))

    started = []

    def gate_up(x, part, sem_l, sem_r):
        for e in range(2):
            both = W.at[e, :, part]
            pltpu.make_async_copy(both, both, sem_l if e == 0 else sem_r).wait()
            for i in range(2):
                y = jnp.dot(x, W[e, i, part, :], preferred_element_type=F32)
                ACC[i, e] = ACC[i, e] + y if started else y
        started.append(1)

    def gate_up_step(key):
        kind, n = key
        for dep in jobs[key][2]:
            hear(dep)
        own_ready(kind[1], n)
        if kind == "ga":
            gate_up(XA[n].reshape(NX * rows, ka), rows_a[n], wla_sem.at[n], wra_sem.at[n])
        else:
            gate_up(XB[n].reshape(NX * rows, kb), rows_b[n], wlb_sem.at[n], wrb_sem.at[n])

    pushes, clock = [], 0.0
    for need, (kind, n) in [(t, key) for t, key in order if jobs[key][0] == 4]:
        for i in range(2):
            pushes.append((min(clock, need - 3.0), "w", (kind, n, i)))
            clock += (ka if kind == "ga" else kb) * hid * 2 / cfg["push_rate"]
    for p in range(NY):
        pushes.append((clock, "d", p))
        clock += ncol * hid * 2 / cfg["push_rate"]
    dr = []

    def push(kind, what):
        if kind == "d":
            dr.append(remote(wd_ref.at[0, :, dcols[what]], WD.at[what, pl.ds(hid, hid)], D_SEND, dr_recv.at[what], partner))
            return
        group, n, i = what
        src, dst, sem = (rows_a[n], rows_a[n], wra_sem.at[n]) if group == "ga" else (from_b[n], rows_b[n], wrb_sem.at[n])
        remote((wg_ref, wu_ref)[i].at[0, src], W.at[1, i, dst], W_SEND, sem, partner)

    events = sorted([(t, 1, n, ("s", key)) for n, (t, key) in enumerate(order)]
                    + [(t, 0, n, (kind, what)) for n, (t, kind, what) in enumerate(pushes)])
    for _, _, _, (kind, what) in events:
        if kind != "s":
            push(kind, what)
        elif jobs[what][0] == 4:
            gate_up_step(what)
        else:
            send(what)
    for d in range(2):
        for st in range(HX):
            hear(("g", 0, st, d))

    g_all = G[...].reshape(NX * rows, 128).astype(F32)
    glane = lax.broadcasted_iota(jnp.int32, (NX * rows, 128), 1)
    grow = lax.broadcasted_iota(jnp.int32, (NX * rows, 128), 0)
    tally = jnp.where((glane == 2 * nexp) & (grow % rows == 0), g_all, 0.0)
    C[0] = jnp.zeros((8, 128), F32) + jnp.sum(tally)
    c_copy = remote(C.at[0], C.at[1], C_SEND, c_recv, partner)
    hs = []
    for e in range(2):
        expert = ep if e == 0 else partner["ep"]
        gate = jnp.sum(jnp.where((glane == expert) | (glane == expert + nexp), g_all, 0.0), axis=1, keepdims=True)
        g, u = ACC[0, e], ACC[1, e]
        hs.append((gate * (g / (1.0 + jnp.exp(-g)) * u)).astype(BF16))
    h = jnp.concatenate(hs, axis=1)

    def down(p):
        dl[p].wait()
        dr[p].wait_recv()
        y = jnp.dot(h, WD[p], preferred_element_type=F32).astype(BF16).reshape(NX, rows, ncol)
        P1[p] = y[:, :half]
        P2[p] = y[:, half:]

    pos = {k: p for p, k in enumerate(kk)}
    NQ, NJ = NY // 2, NX // 2
    last = NY - 1
    jobs2 = scatter_jobs(NX, NY, NQ, NJ, kk, cfg["us_unit"], cfg["us_down"])
    sent = {}
    done = set()

    def once(key):
        if key in done:
            return False
        done.add(key)
        return True

    def add(dst, *srcs):
        total = dst[...].astype(F32)
        for src in srcs:
            total = total + src[...].astype(F32)
        dst[...] = total.astype(BF16)

    def h1_step(q, s, d):
        slot = (HX + s) % NX if d == 0 else HX - s
        if s == 0:
            p, n = 2 * q + d, 1
        else:
            p, n = 2 * q, 2
            sent["h1", q, s - 1, d].wait_recv()
            pa, na = (2 * q + d, 1) if s == 1 else (p, n)
            add(P1.at[pl.ds(pa, na), slot], RB1.at[d, s - 1, pl.ds(pa, na)])
        sent["h1", q, s, d] = remote(P1.at[pl.ds(p, n), slot], RB1.at[d, s, pl.ds(p, n)], H1_SEND, h1_recv.at[q, s, d],
                                     xdev(1 if d == 0 else -1))

    def h2_step(j, s, d):
        p = pos[HY - s] if (d == 0 or s == 0) else pos[s - HY]
        rng = pl.ds(2 * j, 2)
        if ("h2", j, s - 1, d) in sent:
            sent["h2", j, s - 1, d].wait_recv()
            add(P2.at[p, rng], RB2.at[d, s - 1, rng])
        sent["h2", j, s, d] = remote(P2.at[p, rng], RB2.at[d, s, rng], H2_SEND, h2_recv.at[j, s, d], ydev(1 if d == 0 else -1))

    def h1_final(q):
        if once(("h1", q)):
            sent["h1", q, HX - 1, 0].wait_recv()
            sent["h1", q, HX - 1, 1].wait_recv()
            r = pl.ds(2 * q, 2)
            add(P1.at[r, 0], RB1.at[0, HX - 1, r], RB1.at[1, HX - 1, r])

    def h2_final(j):
        if once(("h2", j)):
            sent["h2", j, HY - 1, 0].wait_recv()
            sent["h2", j, HY - 1, 1].wait_recv()
            r = pl.ds(2 * j, 2)
            add(P2.at[last, r], RB2.at[0, HY - 1, r], RB2.at[1, HY - 1, r])

    f1, f2 = [], []
    cut = -(-(ncol // 128) // 2) * 128
    parts = (pl.ds(0, cut), pl.ds(cut, ncol - cut))
    for _, key in plan(jobs2, cfg["lat2"]):
        if key[0] == "down":
            down(key[1])
        elif key[0] == "h1":
            h1_step(*key[1:])
        elif key[0] == "h2":
            h2_step(*key[1:])
        elif key[0] == "e1":
            d = key[1]
            h1_final(pos[HY] // 2)
            sent[key] = remote(P1.at[pos[HY], 0, :, parts[d]], E.at[0, :, parts[d]], E_SEND, e_recv.at[0, d],
                               ydev(1 if d == 0 else -1))
        elif key[0] == "e2":
            d = key[1]
            h2_final(HX // 2)
            sent[key] = remote(P2.at[last, HX, :, parts[d]], E.at[1, :, parts[d]], E_SEND, e_recv.at[1, d],
                               xdev(-1 if d == 0 else 1))
        elif key[0] == "f1":
            p = key[1]
            h1_final(p // 2)
            if abs(kk[p]) == HY - 1:
                d = 0 if kk[p] > 0 else 1
                sent["e1", d].wait_recv()
                add(P1.at[p, 0, :, parts[d]], E.at[0, :, parts[d]])
            f1.append((p, remote(P1.at[p, 0], F1.at[p], F1_SEND, f1_recv.at[p], ydev(kk[p]))))
        else:
            slot = key[1]
            h2_final(slot // 2)
            if min(slot, NX - slot) == HX - 1:
                d = 0 if slot < HX else 1
                sent["e2", d].wait_recv()
                add(P2.at[last, slot, :, parts[d]], E.at[1, :, parts[d]])
            f2.append((slot, remote(P2.at[last, slot], F2.at[slot], F2_SEND, f2_recv.at[slot], xdev(-slot))))

    for q in range(NQ):
        h1_final(q)
    for j in range(NJ):
        h2_final(j)
    for n, (own, arrived, ref) in enumerate(((P1.at[last, 0], f1, F1), (P2.at[last, 0], f2, F2))):
        total = own[...].astype(F32)
        for m, c in arrived:
            c.wait_recv()
            total = total + ref[m].astype(F32)
        out_ref[pl.ds(n * half, half), :] = total.astype(BF16)
    c_copy.wait_recv()
    first_only = ((lax.broadcasted_iota(jnp.int32, (8, 128), 0) == 0)
                  & (lax.broadcasted_iota(jnp.int32, (8, 128), 1) == 0))
    count_ref[0] = jnp.sum(jnp.where(first_only, C[0] + C[1], 0.0)).astype(jnp.int32)

    def drained(sem, ref):
        pltpu.make_async_copy(ref, ref, send_sem.at[sem]).wait()

    most = pl.ds(0, NX - 1)
    drained(A_SEND, XA.at[:, most])
    drained(B_SEND, XB.at[0, most])
    drained(G_SEND, G.at[most])
    drained(Y_SEND, XB.at[pl.ds(0, 3), most])
    drained(W_SEND, W.at[1])
    drained(D_SEND, WD.at[:, pl.ds(0, hid)])
    drained(C_SEND, C.at[0])
    drained(H1_SEND, P1.at[:, most])
    drained(H2_SEND, P2.at[pl.ds(0, NY - 1)])
    drained(E_SEND, E)
    drained(F1_SEND, F1.at[pl.ds(0, NY - 2)])
    drained(F2_SEND, F2.at[pl.ds(0, NX - 2)])


def per_device(tokens, w_gate, w_up, w_down, router_logits, expert_ids, draft_lengths, accept_mask):
    nx, ny = lax.axis_size("ep") // 2, lax.axis_size("tp")
    rows, width = tokens.shape
    hid = w_gate.shape[2]
    ncol = width // ny
    half = rows // 2
    hx, hy = nx // 2, ny // 2
    nb, nsub, kb = 4, 2, 1024
    na = 3
    ka = (width - nb * kb) // na
    us_per_col = rows * 2 / 46.6e3
    cfg = dict(nx=nx, ny=ny, na=na, ka=ka, nb=nb, nsub=nsub, kb=kb, rows=rows, ncol=ncol, hid=hid,
               nexp=lax.axis_size("ep"), us_per_col=us_per_col, us_dot=0.6e-3, lat=3.0, push_rate=450e3,
               us_unit=half * ncol * 2 / 46.6e3, us_down=0.27, lat2=2.4)
    dma = pltpu.SemaphoreType.DMA
    scratch = [
        pltpu.VMEM((na, nx, rows, ka), BF16),
        pltpu.VMEM((nb, nx, rows, kb), BF16),
        pltpu.VMEM((nx, rows, 128), BF16),
        pltpu.VMEM((2, 2, width, hid), BF16),
        pltpu.VMEM((ny, 2 * hid, ncol), BF16),
        pltpu.VMEM((2, 2, nx * rows, hid), F32),
        pltpu.VMEM((ny, nx, half, ncol), BF16),
        pltpu.VMEM((ny, nx, half, ncol), BF16),
        pltpu.VMEM((2, hx, ny, half, ncol), BF16),
        pltpu.VMEM((2, hy, nx, half, ncol), BF16),
        pltpu.VMEM((ny, half, ncol), BF16),
        pltpu.VMEM((nx, half, ncol), BF16),
        pltpu.VMEM((2, half, ncol), BF16),
        pltpu.VMEM((2, 8, 128), F32),
        dma((na,)), dma((nb,)), dma((na,)), dma((nb,)), dma((na,)), dma((nb,)),
        dma((na, hx, 2)), dma((nsub, hx, 2)), dma((hx, 2)), dma((nsub, nx, 2, 2)), dma((ny // 2, hx, 2)), dma((nx // 2, hy, 2)),
        dma((ny,)), dma((nx,)), dma((2, 2)), dma(()), dma((ny,)), dma((ny,)), dma((12,)),
    ]
    anyspec = pl.BlockSpec(memory_space=pl.ANY)
    vmem = pl.BlockSpec(memory_space=pltpu.VMEM)
    smem = pl.BlockSpec(memory_space=pltpu.SMEM)
    mixed, accepted = pl.pallas_call(
        functools.partial(kernel, cfg),
        out_shape=(pltpu.VMEM((rows, ncol), BF16), jax.ShapeDtypeStruct((1,), jnp.int32)),
        in_specs=[anyspec] * 4 + [vmem, vmem, smem, vmem],
        out_specs=(vmem, smem),
        scratch_shapes=scratch,
        name="routed_experts",
        compiler_params=pltpu.CompilerParams(collective_id=0, has_side_effects=True, vmem_limit_bytes=60 * 1024 * 1024),
    )(tokens, w_gate, w_up, w_down, router_logits.T, expert_ids.T, draft_lengths, accept_mask)
    return mixed, accepted


def solution(mesh):
    placed = (
        P(("groups", "ep"), None),
        P("ep", None, "tp"),
        P("ep", None, "tp"),
        P("ep", "tp", None),
        P(("groups", "ep"), None),
        P(("groups", "ep"), None),
        P(("groups", "ep")),
        P(("groups", "ep"), None),
    )
    return jax.shard_map(
        per_device,
        mesh=mesh,
        in_specs=placed,
        out_specs=(P(("groups", "ep"), "tp"), P("groups")),
        check_vma=False,
    )
```

```python
import functools

import jax
import jax.numpy as jnp
from jax import lax
from jax.experimental import pallas as pl
from jax.experimental.pallas import tpu as pltpu
from jax.sharding import PartitionSpec as P

MESH = pl.DeviceIdType.MESH
DRAFT = 8
SCALE = 2.827
BF16, F32 = jnp.bfloat16, jnp.float32


def signed_order(n):
    half = n // 2
    order = [half]
    for d in range(half - 1, 0, -1):
        order += [d, -d]
    return order + [0]


def gather_jobs(nx, na, ka, nb, nsub, kb, us_per_col, us_dot):
    hx = nx // 2
    jobs = {}
    for st in range(hx):
        cut = 0.5 if st == hx - 1 else 1.0
        for d in range(2):
            for q in range(na):
                jobs["a", q, st, d] = (d, ka * us_per_col * cut, [("a", q, st - 1, d)] if st else [], 100 + q)
            for n in range(nsub):
                jobs["b", n, st, d] = (d, kb / nsub * us_per_col * cut, [("b", n, st - 1, d)] if st else [], 0.1 * n)
            jobs["g", 0, st, d] = (d, 128 * us_per_col * cut, [("g", 0, st - 1, d)] if st else [], 1)
    for j in range(1, nx):
        for n in range(nsub):
            dep = [("b", n, st, d) for st, d in ((j - 1, 0), (nx - 1 - j, 1)) if st < hx]
            for d in range(2):
                far = min(j, nx - j)
                jobs["y", n, j, 0, d] = (2 + d, kb / nsub * us_per_col, dep, 10 - far)
                jobs["y", n, j, 1, d] = (2 + d, kb / nsub * us_per_col / 2, [("y", n, j, 0, d)], 9 - far)
    for q in range(na):
        jobs["ga", q] = (4, us_dot * ka, [("a", q, st, d) for st in range(hx) for d in range(2)], 500)
    slots, subs = range(1, nx), range(nsub)
    for r in range(nb):
        if r == 0:
            deps = [("b", n, st, d) for n in subs for st in range(hx) for d in range(2)]
        elif r == 2:
            deps = [("y", n, j, 1, d) for n in subs for j in slots for d in range(2)]
        else:
            deps = [("y", n, j, 0, 0 if r == 3 else 1) for n in subs for j in slots]
        jobs["gb", r] = (4, us_dot * kb, deps, 500)
    return jobs


def scatter_jobs(nx, ny, nq, nj, kk, us_unit, us_down):
    hx, hy = nx // 2, ny // 2
    pos = {k: p for p, k in enumerate(kk)}
    jobs = {("down", p): (4, us_down, [("down", p - 1)] if p else [], p) for p in range(ny)}
    for q in range(nq):
        for st in range(hx):
            for d in range(2):
                deps = [("down", 2 * q + d)] if st == 0 else [("h1", q, st - 1, d), ("down", 2 * q), ("down", 2 * q + 1)]
                jobs["h1", q, st, d] = (d, us_unit * (1 if st == 0 else 2), deps, 600 + st * 10 + q)
        ready = [("h1", q, hx - 1, 0), ("h1", q, hx - 1, 1)]
        for p in (2 * q, 2 * q + 1):
            far = abs(kk[p])
            if far == hy:
                for d in range(2):
                    jobs["e1", d] = (2 + d, us_unit / 2, ready, 500)
            elif far:
                relay = [("e1", 0 if kk[p] > 0 else 1)] if far == hy - 1 else []
                jobs["f1", p] = (2 if kk[p] > 0 else 3, us_unit * far, ready + relay, 700 - far)
    by_distance = sorted(range(nj), key=lambda j: (-max(min(m, nx - m) for m in (2 * j, 2 * j + 1)), j))
    for j in range(nj):
        for st in range(hy):
            for d in range(2):
                mine = (j < nj // 2) == (d == 0)
                if st == 0 and not mine:
                    continue
                deps = [("down", pos[hy - st] if (d == 0 or st == 0) else pos[st - hy])]
                if st > 1 or (st == 1 and mine):
                    deps.append(("h2", j, st - 1, d))
                jobs["h2", j, st, d] = (2 + d, us_unit * 2, deps, 600 + st * 10 + by_distance.index(j))
        ready = [("h2", j, hy - 1, 0), ("h2", j, hy - 1, 1), ("down", ny - 1)]
        for slot in (2 * j, 2 * j + 1):
            far = min(slot, nx - slot)
            if far == hx:
                for d in range(2):
                    jobs["e2", d] = (1 - d, us_unit / 2, ready, 500)
            elif far:
                relay = [("e2", 0 if slot < hx else 1)] if far == hx - 1 else []
                jobs["f2", slot] = (1 if slot < hx else 0, us_unit * far, ready + relay, 700 - far)
    return jobs


def plan(jobs, lat):
    missing = {k: len(v[2]) for k, v in jobs.items()}
    users = {}
    for k, v in jobs.items():
        for dep in v[2]:
            users.setdefault(dep, []).append(k)
    resources = range(5)
    able = {r: [k for k in jobs if jobs[k][0] == r and not missing[k]] for r in resources}
    when = {k: 0.0 for k in jobs}
    free, order = [0.0 for _ in resources], []
    while len(order) < len(jobs):
        best = None
        for r in resources:
            if able[r]:
                t = max(free[r], min(when[k] for k in able[r]))
                k = min((k for k in able[r] if when[k] <= t + 1e-9), key=lambda k: (jobs[k][3], when[k], k))
                if best is None or t < best[0]:
                    best = (t, k)
        t, k = best
        r = jobs[k][0]
        able[r].remove(k)
        free[r] = t + jobs[k][1]
        order.append((t, k))
        for m in users.get(k, []):
            when[m] = max(when[m], free[r] + (0.0 if r == 4 else lat))
            missing[m] -= 1
            if not missing[m]:
                able[jobs[m][0]].append(m)
    return order


def kernel(cfg, tok_ref, wg_ref, wu_ref, wd_ref, logit_ref, ids_ref, len_ref, mask_ref, out_ref, count_ref,
           XA, XB, G, W, WD, ACC, P1, P2, RB1, RB2, F1, F2, E, C,
           ta_sem, tb_sem, wla_sem, wlb_sem, wra_sem, wrb_sem, a_recv, b_recv, g_recv, y_recv, h1_recv, h2_recv,
           f1_recv, f2_recv, e_recv, c_recv, d_sem, dr_recv, send_sem):
    NX, NY, NA, NB, NSUB = cfg["nx"], cfg["ny"], cfg["na"], cfg["nb"], cfg["nsub"]
    HX, HY = NX // 2, NY // 2
    rows = cfg["rows"]
    half = rows // 2
    ka, kb = cfg["ka"], cfg["kb"]
    ncol = cfg["ncol"]
    hid = cfg["hid"]
    nexp = cfg["nexp"]
    n_ep = 2 * NX
    base = NA * ka
    ep = lax.axis_index("ep")
    tp = lax.axis_index("tp")
    core = lax.rem(ep, 2)
    partner = {"ep": ep + 1 - 2 * core}

    def xdev(d):
        there = lax.rem(ep + (2 * d) % n_ep, n_ep)
        return {"ep": there + 1 - 2 * core if d % 2 else there}

    def ydev(d):
        return {"tp": lax.rem(tp + d % NY, NY)}

    def slice_of(r, count, size, start=0):
        return pl.ds(pl.multiple_of(start + lax.rem(tp + r % count, count) * size, 128), size)

    kk = signed_order(NY)
    A_SEND, B_SEND, G_SEND, Y_SEND, H1_SEND, H2_SEND, F1_SEND, F2_SEND, C_SEND, W_SEND, D_SEND, E_SEND = range(12)

    def remote(src, dst, send, recv, dev):
        c = pltpu.make_async_remote_copy(src_ref=src, dst_ref=dst, send_sem=send_sem.at[send], recv_sem=recv,
                                         device_id=dev, device_id_type=MESH)
        c.start()
        return c

    barrier = pltpu.get_barrier_semaphore()
    peers = [partner, xdev(1), xdev(-1), ydev(1), ydev(-1)]
    for dev in peers:
        pl.semaphore_signal(barrier, inc=1, device_id=dev, device_id_type=MESH)

    tok_a, tok_b = [], []
    for r in range(NB):
        c = pltpu.make_async_copy(tok_ref.at[:, slice_of(r, NB, kb, base)], XB.at[r, 0], tb_sem.at[r])
        c.start()
        tok_b.append(c)
    for q in range(NA):
        c = pltpu.make_async_copy(tok_ref.at[:, pl.ds(q * ka, ka)], XA.at[q, 0], ta_sem.at[q])
        c.start()
        tok_a.append(c)
    rows_a = [pl.ds(q * ka, ka) for q in range(NA)]
    rows_b = [pl.ds(base + r * kb, kb) for r in range(NB)]
    from_b = [slice_of(r, NB, kb, base) for r in range(NB)]
    for src, dst, sem in ([(rows_a[q], rows_a[q], wla_sem.at[q]) for q in range(NA)]
                          + [(from_b[r], rows_b[r], wlb_sem.at[r]) for r in range(NB)]):
        for i, w in enumerate((wg_ref, wu_ref)):
            pltpu.make_async_copy(w.at[0, src], W.at[0, i, dst], sem).start()
    dl = []
    dcols = []
    for p in range(NY):
        dcols.append(slice_of(kk[p], NY, ncol))
        c = pltpu.make_async_copy(wd_ref.at[0, :, dcols[p]], WD.at[p, pl.ds(0, hid)], d_sem.at[p])
        c.start()
        dl.append(c)

    def own_gates():
        logits = logit_ref[...]
        sig = 1.0 / (1.0 + jnp.exp(-logits))
        gates = SCALE * sig / jnp.sum(sig, axis=0, keepdims=True)
        lane = lax.broadcasted_iota(jnp.int32, (1, rows), 1)
        length = jnp.zeros((1, rows), jnp.int32)
        for r in range(rows // DRAFT):
            length = jnp.where(lane // DRAFT == r, len_ref[r], length)
        gates = jnp.where(lane % DRAFT < length, gates, 0.0)
        mrow = lax.broadcasted_iota(jnp.int32, mask_ref.shape, 0)
        mcol = lax.broadcasted_iota(jnp.int32, mask_ref.shape, 1)
        mlen = jnp.zeros(mask_ref.shape, jnp.int32)
        for r in range(rows // DRAFT):
            mlen = jnp.where(mrow == r, len_ref[r], mlen)
        passed = jnp.where(mcol < mlen, mask_ref[...], 0).astype(F32)
        run = passed[:, 0:1]
        local_count = run
        for j in range(1, DRAFT):
            run = run * passed[:, j:j + 1]
            local_count = local_count + run
        local_count = jnp.sum(local_count, axis=0, keepdims=True)
        feat = lax.broadcasted_iota(jnp.int32, (128, rows), 0)
        dense = jnp.zeros((128, rows), F32)
        ids = ids_ref[...]
        for k in range(ids.shape[0]):
            e = ids[k:k + 1, :]
            dense = dense + jnp.where((feat == e) | (feat == e + nexp), gates[k:k + 1, :], 0.0)
        high = dense.astype(BF16)
        packed = jnp.where(feat < nexp, high.astype(F32), dense - high.astype(F32))
        packed = packed + jnp.where(feat == 2 * nexp, local_count, 0.0)
        eye = (lax.broadcasted_iota(jnp.int32, (rows, rows), 0) == lax.broadcasted_iota(jnp.int32, (rows, rows), 1))
        turned = lax.dot_general(eye.astype(F32).astype(BF16), packed.astype(BF16), (((1,), (1,)), ((), ())),
                                 preferred_element_type=F32)
        G[0] = turned.astype(BF16)

    pl.semaphore_wait(barrier, len(peers))

    lo, hi = pl.ds(0, half), pl.ds(half, half)
    jobs = gather_jobs(NX, NA, ka, NB, NSUB, kb, cfg["us_per_col"], cfg["us_dot"])
    order = plan(jobs, cfg["lat"])
    copies = {}
    heard = set()

    def hear(key):
        if key not in heard:
            heard.add(key)
            copies[key].wait_recv()

    def own_ready(kind, n):
        if (kind, n) not in heard:
            heard.add((kind, n))
            (tok_a if kind == "a" else tok_b)[n].wait()

    def send(key):
        kind, n, st, d = key[0], key[1], key[-2], key[-1]
        for dep in jobs[key][2]:
            hear(dep)
        part = lo if d == 0 else hi
        cols = pl.ds(n * (kb // NSUB), kb // NSUB)
        if kind == "y":
            j = key[2]
            r, to = ((0, 3), (3, 2))[st] if d == 0 else ((0, 1), (1, 2))[st]
            take = part if st == 1 else pl.ds(0, rows)
            copies[key] = remote(XB.at[r, j, take, cols], XB.at[to, j, take, cols], Y_SEND, y_recv.at[n, j, st, d],
                                 ydev(1 if d == 0 else -1))
            return
        a, b = (st, st + 1) if d == 0 else ((NX - st) % NX, NX - st - 1)
        take = part if st == HX - 1 else pl.ds(0, rows)
        if kind == "a":
            own_ready("a", n)
            src, dst, sem, recv = XA.at[n, a, take], XA.at[n, b, take], A_SEND, a_recv.at[n, st, d]
        elif kind == "b":
            own_ready("b", 0)
            src, dst, sem, recv = XB.at[0, a, take, cols], XB.at[0, b, take, cols], B_SEND, b_recv.at[n, st, d]
        else:
            if "gates" not in heard:
                heard.add("gates")
                own_gates()
            src, dst, sem, recv = G.at[a, take], G.at[b, take], G_SEND, g_recv.at[st, d]
        copies[key] = remote(src, dst, sem, recv, xdev(1 if d == 0 else -1))

    started = []

    def gate_up(x, part, sem_l, sem_r):
        for e in range(2):
            both = W.at[e, :, part]
            pltpu.make_async_copy(both, both, sem_l if e == 0 else sem_r).wait()
            for i in range(2):
                y = jnp.dot(x, W[e, i, part, :], preferred_element_type=F32)
                ACC[i, e] = ACC[i, e] + y if started else y
        started.append(1)

    def gate_up_step(key):
        kind, n = key
        for dep in jobs[key][2]:
            hear(dep)
        own_ready(kind[1], n)
        if kind == "ga":
            gate_up(XA[n].reshape(NX * rows, ka), rows_a[n], wla_sem.at[n], wra_sem.at[n])
        else:
            gate_up(XB[n].reshape(NX * rows, kb), rows_b[n], wlb_sem.at[n], wrb_sem.at[n])

    pushes, clock = [], 0.0
    for need, (kind, n) in [(t, key) for t, key in order if jobs[key][0] == 4]:
        for i in range(2):
            pushes.append((min(clock, need - 3.0), "w", (kind, n, i)))
            clock += (ka if kind == "ga" else kb) * hid * 2 / cfg["push_rate"]
    for p in range(NY):
        pushes.append((clock, "d", p))
        clock += ncol * hid * 2 / cfg["push_rate"]
    dr = []

    def push(kind, what):
        if kind == "d":
            dr.append(remote(wd_ref.at[0, :, dcols[what]], WD.at[what, pl.ds(hid, hid)], D_SEND, dr_recv.at[what], partner))
            return
        group, n, i = what
        src, dst, sem = (rows_a[n], rows_a[n], wra_sem.at[n]) if group == "ga" else (from_b[n], rows_b[n], wrb_sem.at[n])
        remote((wg_ref, wu_ref)[i].at[0, src], W.at[1, i, dst], W_SEND, sem, partner)

    events = sorted([(t, 1, n, ("s", key)) for n, (t, key) in enumerate(order)]
                    + [(t, 0, n, (kind, what)) for n, (t, kind, what) in enumerate(pushes)])
    for _, _, _, (kind, what) in events:
        if kind != "s":
            push(kind, what)
        elif jobs[what][0] == 4:
            gate_up_step(what)
        else:
            send(what)
    for d in range(2):
        for st in range(HX):
            hear(("g", 0, st, d))

    g_all = G[...].reshape(NX * rows, 128).astype(F32)
    glane = lax.broadcasted_iota(jnp.int32, (NX * rows, 128), 1)
    grow = lax.broadcasted_iota(jnp.int32, (NX * rows, 128), 0)
    tally = jnp.where((glane == 2 * nexp) & (grow % rows == 0), g_all, 0.0)
    C[0] = jnp.zeros((8, 128), F32) + jnp.sum(tally)
    c_copy = remote(C.at[0], C.at[1], C_SEND, c_recv, partner)
    hs = []
    for e in range(2):
        expert = ep if e == 0 else partner["ep"]
        gate = jnp.sum(jnp.where((glane == expert) | (glane == expert + nexp), g_all, 0.0), axis=1, keepdims=True)
        g, u = ACC[0, e], ACC[1, e]
        hs.append((gate * (g / (1.0 + jnp.exp(-g)) * u)).astype(BF16))
    h = jnp.concatenate(hs, axis=1)

    def down(p):
        dl[p].wait()
        dr[p].wait_recv()
        y = jnp.dot(h, WD[p], preferred_element_type=F32).astype(BF16).reshape(NX, rows, ncol)
        P1[p] = y[:, :half]
        P2[p] = y[:, half:]

    pos = {k: p for p, k in enumerate(kk)}
    NQ, NJ = NY // 2, NX // 2
    last = NY - 1
    jobs2 = scatter_jobs(NX, NY, NQ, NJ, kk, cfg["us_unit"], cfg["us_down"])
    sent = {}
    done = set()

    def once(key):
        if key in done:
            return False
        done.add(key)
        return True

    def add(dst, *srcs):
        total = dst[...].astype(F32)
        for src in srcs:
            total = total + src[...].astype(F32)
        dst[...] = total.astype(BF16)

    def h1_step(q, s, d):
        slot = (HX + s) % NX if d == 0 else HX - s
        if s == 0:
            p, n = 2 * q + d, 1
        else:
            p, n = 2 * q, 2
            sent["h1", q, s - 1, d].wait_recv()
            pa, na = (2 * q + d, 1) if s == 1 else (p, n)
            add(P1.at[pl.ds(pa, na), slot], RB1.at[d, s - 1, pl.ds(pa, na)])
        sent["h1", q, s, d] = remote(P1.at[pl.ds(p, n), slot], RB1.at[d, s, pl.ds(p, n)], H1_SEND, h1_recv.at[q, s, d],
                                     xdev(1 if d == 0 else -1))

    def h2_step(j, s, d):
        p = pos[HY - s] if (d == 0 or s == 0) else pos[s - HY]
        rng = pl.ds(2 * j, 2)
        if ("h2", j, s - 1, d) in sent:
            sent["h2", j, s - 1, d].wait_recv()
            add(P2.at[p, rng], RB2.at[d, s - 1, rng])
        sent["h2", j, s, d] = remote(P2.at[p, rng], RB2.at[d, s, rng], H2_SEND, h2_recv.at[j, s, d], ydev(1 if d == 0 else -1))

    def h1_final(q):
        if once(("h1", q)):
            sent["h1", q, HX - 1, 0].wait_recv()
            sent["h1", q, HX - 1, 1].wait_recv()
            r = pl.ds(2 * q, 2)
            add(P1.at[r, 0], RB1.at[0, HX - 1, r], RB1.at[1, HX - 1, r])

    def h2_final(j):
        if once(("h2", j)):
            sent["h2", j, HY - 1, 0].wait_recv()
            sent["h2", j, HY - 1, 1].wait_recv()
            r = pl.ds(2 * j, 2)
            add(P2.at[last, r], RB2.at[0, HY - 1, r], RB2.at[1, HY - 1, r])

    f1, f2 = [], []
    cut = -(-(ncol // 128) // 2) * 128
    parts = (pl.ds(0, cut), pl.ds(cut, ncol - cut))
    for _, key in plan(jobs2, cfg["lat2"]):
        if key[0] == "down":
            down(key[1])
        elif key[0] == "h1":
            h1_step(*key[1:])
        elif key[0] == "h2":
            h2_step(*key[1:])
        elif key[0] == "e1":
            d = key[1]
            h1_final(pos[HY] // 2)
            sent[key] = remote(P1.at[pos[HY], 0, :, parts[d]], E.at[0, :, parts[d]], E_SEND, e_recv.at[0, d],
                               ydev(1 if d == 0 else -1))
        elif key[0] == "e2":
            d = key[1]
            h2_final(HX // 2)
            sent[key] = remote(P2.at[last, HX, :, parts[d]], E.at[1, :, parts[d]], E_SEND, e_recv.at[1, d],
                               xdev(-1 if d == 0 else 1))
        elif key[0] == "f1":
            p = key[1]
            h1_final(p // 2)
            if abs(kk[p]) == HY - 1:
                d = 0 if kk[p] > 0 else 1
                sent["e1", d].wait_recv()
                add(P1.at[p, 0, :, parts[d]], E.at[0, :, parts[d]])
            f1.append((p, remote(P1.at[p, 0], F1.at[p], F1_SEND, f1_recv.at[p], ydev(kk[p]))))
        else:
            slot = key[1]
            h2_final(slot // 2)
            if min(slot, NX - slot) == HX - 1:
                d = 0 if slot < HX else 1
                sent["e2", d].wait_recv()
                add(P2.at[last, slot, :, parts[d]], E.at[1, :, parts[d]])
            f2.append((slot, remote(P2.at[last, slot], F2.at[slot], F2_SEND, f2_recv.at[slot], xdev(-slot))))

    for q in range(NQ):
        h1_final(q)
    for j in range(NJ):
        h2_final(j)
    for n, (own, arrived, ref) in enumerate(((P1.at[last, 0], f1, F1), (P2.at[last, 0], f2, F2))):
        total = own[...].astype(F32)
        for m, c in arrived:
            c.wait_recv()
            total = total + ref[m].astype(F32)
        out_ref[pl.ds(n * half, half), :] = total.astype(BF16)
    c_copy.wait_recv()
    first_only = ((lax.broadcasted_iota(jnp.int32, (8, 128), 0) == 0)
                  & (lax.broadcasted_iota(jnp.int32, (8, 128), 1) == 0))
    count_ref[0] = jnp.sum(jnp.where(first_only, C[0] + C[1], 0.0)).astype(jnp.int32)

    def drained(sem, ref):
        pltpu.make_async_copy(ref, ref, send_sem.at[sem]).wait()

    most = pl.ds(0, NX - 1)
    drained(A_SEND, XA.at[:, most])
    drained(B_SEND, XB.at[0, most])
    drained(G_SEND, G.at[most])
    drained(Y_SEND, XB.at[pl.ds(0, 3), most])
    drained(W_SEND, W.at[1])
    drained(D_SEND, WD.at[:, pl.ds(0, hid)])
    drained(C_SEND, C.at[0])
    drained(H1_SEND, P1.at[:, most])
    drained(H2_SEND, P2.at[pl.ds(0, NY - 1)])
    drained(E_SEND, E)
    drained(F1_SEND, F1.at[pl.ds(0, NY - 2)])
    drained(F2_SEND, F2.at[pl.ds(0, NX - 2)])


def per_device(tokens, w_gate, w_up, w_down, router_logits, expert_ids, draft_lengths, accept_mask):
    nx, ny = lax.axis_size("ep") // 2, lax.axis_size("tp")
    rows, width = tokens.shape
    hid = w_gate.shape[2]
    ncol = width // ny
    half = rows // 2
    hx, hy = nx // 2, ny // 2
    nb, nsub, kb = 4, 3, 1152
    na = 2
    ka = (width - nb * kb) // na
    us_per_col = rows * 2 / 46.6e3
    cfg = dict(nx=nx, ny=ny, na=na, ka=ka, nb=nb, nsub=nsub, kb=kb, rows=rows, ncol=ncol, hid=hid,
               nexp=lax.axis_size("ep"), us_per_col=us_per_col, us_dot=0.6e-3, lat=2.8, push_rate=450e3,
               us_unit=half * ncol * 2 / 46.6e3, us_down=0.27, lat2=2.4)
    dma = pltpu.SemaphoreType.DMA
    scratch = [
        pltpu.VMEM((na, nx, rows, ka), BF16),
        pltpu.VMEM((nb, nx, rows, kb), BF16),
        pltpu.VMEM((nx, rows, 128), BF16),
        pltpu.VMEM((2, 2, width, hid), BF16),
        pltpu.VMEM((ny, 2 * hid, ncol), BF16),
        pltpu.VMEM((2, 2, nx * rows, hid), F32),
        pltpu.VMEM((ny, nx, half, ncol), BF16),
        pltpu.VMEM((ny, nx, half, ncol), BF16),
        pltpu.VMEM((2, hx, ny, half, ncol), BF16),
        pltpu.VMEM((2, hy, nx, half, ncol), BF16),
        pltpu.VMEM((ny, half, ncol), BF16),
        pltpu.VMEM((nx, half, ncol), BF16),
        pltpu.VMEM((2, half, ncol), BF16),
        pltpu.VMEM((2, 8, 128), F32),
        dma((na,)), dma((nb,)), dma((na,)), dma((nb,)), dma((na,)), dma((nb,)),
        dma((na, hx, 2)), dma((nsub, hx, 2)), dma((hx, 2)), dma((nsub, nx, 2, 2)), dma((ny // 2, hx, 2)), dma((nx // 2, hy, 2)),
        dma((ny,)), dma((nx,)), dma((2, 2)), dma(()), dma((ny,)), dma((ny,)), dma((12,)),
    ]
    anyspec = pl.BlockSpec(memory_space=pl.ANY)
    vmem = pl.BlockSpec(memory_space=pltpu.VMEM)
    smem = pl.BlockSpec(memory_space=pltpu.SMEM)
    mixed, accepted = pl.pallas_call(
        functools.partial(kernel, cfg),
        out_shape=(pltpu.VMEM((rows, ncol), BF16), jax.ShapeDtypeStruct((1,), jnp.int32)),
        in_specs=[anyspec] * 4 + [vmem, vmem, smem, vmem],
        out_specs=(vmem, smem),
        scratch_shapes=scratch,
        name="routed_experts",
        compiler_params=pltpu.CompilerParams(collective_id=0, has_side_effects=True, vmem_limit_bytes=60 * 1024 * 1024),
    )(tokens, w_gate, w_up, w_down, router_logits.T, expert_ids.T, draft_lengths, accept_mask)
    return mixed, accepted


def solution(mesh):
    placed = (
        P(("groups", "ep"), None),
        P("ep", None, "tp"),
        P("ep", None, "tp"),
        P("ep", "tp", None),
        P(("groups", "ep"), None),
        P(("groups", "ep"), None),
        P(("groups", "ep")),
        P(("groups", "ep"), None),
    )
    return jax.shard_map(
        per_device,
        mesh=mesh,
        in_specs=placed,
        out_specs=(P(("groups", "ep"), "tp"), P("groups")),
        check_vma=False,
    )
```
